256 devices in a mesh: section: 2 (over x_hi), row: 8 (over y, x_lo), col: 16 (over z, core).
Axes of the slice: x: 4 (x_hi: 2, x_lo: 2; x = x_hi * 2 + x_lo), y: 4, z: 8, core: 2. Of those that a mesh axis runs over, the one named last changes fastest.
Arguments:
- images: bfloat16 [2, 8, 48, 128, 256], P('section', None, None, 'row', 'col'), may hold values from -6 to 6
- stem_first: bfloat16 [48, 256], replicated, may hold values from -0.875 to 0.875
- stem_conv: bfloat16 [3, 3, 256, 256], replicated, may hold values from -0.125 to 0.125
- patch_weight: bfloat16 [4096, 1024], P('col'), may hold values from -0.09375 to 0.09375
- position: bfloat16 [64, 32, 1024], P('col', 'row'), may hold values from -6 to 6
- gain_attn: float32 [1024], replicated, may hold values from 0.1 to 1.9
- w_qkv: bfloat16 [3, 1024, 1024], P(None, None, 'col'), may hold values from -0.5 to 0.5
- w_out: bfloat16 [1024, 1024], P('col'), may hold values from -0.1875 to 0.1875
- gain_mlp: float32 [1024], replicated, may hold values from 0.1 to 1.9
- w_up: bfloat16 [1024, 4096], P(None, 'col'), may hold values from -0.1875 to 0.1875
- w_down: bfloat16 [4096, 1024], P('col'), may hold values from -0.09375 to 0.09375
Outputs:
- encoded: bfloat16 [2, 8, 64, 32, 1024], P('section', 'row', 'col')
The draws below stay inside these ranges and needn't reach their ends.
All inputs are finite; a program needn't handle non-finite values.
Results may differ from the reference program's by a relative error of at most 0.024.
The reference program's roundings to bfloat16 on the way count: a program that leaves them out, or rounds other values in their place, can miss the bound.
Values may be sent and summed in bfloat16 or wider, within the bound.
No kernel may reach another device: no remote copies, remote signals or barrier semaphores. Data moves between devices by JAX's collectives and lax.ppermute only.
A program may use at most 64 MiB of HBM per device.

```python
import jax
import jax.numpy as jnp
from jax import lax

D = 1024
HEADS = 16
HD = 64
FF = 4096
C = 256
TCOLS = 64
PF = 4096
TROWS = 32
IMGS = 8
MB = 2
N_COL = 16


def block_levels(own_key, shape, split, low, top_value):
    gain, own = 1.0, jax.random.fold_in(own_key, 6)
    for dim, blocks in split:
        heights = jnp.exp(jax.random.uniform(jax.random.fold_in(own, dim), (blocks,), jnp.float32, low / len(split), top_value / len(split)))
        gain = gain * jnp.repeat(heights, shape[dim] // blocks).reshape([-1 if axis == dim else 1 for axis in range(len(shape))])
    return gain


def noise(key, extent, deviation, bound, cuts=(), dtype=jnp.bfloat16):
    array = jax.random.normal(key, extent, jnp.float32) * deviation
    if len(cuts) > 0:
        array = block_levels(key, extent, cuts, -0.22, 0.18) * array
    return jnp.clip(array, min=-bound, max=bound).astype(dtype)


def setup_inputs(seed: int = 0) -> dict:
    splits = jax.random.split(jax.random.key(seed), 12)
    return {
        "images": noise(splits[0], (MB, IMGS, 48, 4 * TROWS, 4 * TCOLS), 1.0, 6.0, ((0, 2), (3, 8), (4, 16))),
        "stem_first": noise(splits[1], (48, C), 48 ** -0.5, 0.875),
        "stem_conv": noise(splits[2], (3, 3, C, C), (9 * C) ** -0.5, 0.125),
        "patch_weight": noise(splits[3], (PF, D), PF ** -0.5, 0.09375, ((0, 16),)),
        "position": noise(splits[4], (TCOLS, TROWS, D), 1.0, 6.0, ((0, 16), (1, 8))),
        "gain_attn": jnp.clip(1.0 + 0.18 * jax.random.normal(splits[5], (D,), jnp.float32), 0.1, 1.9),
        "w_qkv": noise(splits[6], (3, D, HEADS * HD), (D // 8) ** -0.5, 0.5, ((2, 16),)),
        "w_out": noise(splits[7], (HEADS * HD, D), (HEADS * HD) ** -0.5, 0.1875, ((0, 16),)),
        "gain_mlp": jnp.clip(1.0 + 0.18 * jax.random.normal(splits[8], (D,), jnp.float32), 0.1, 1.9),
        "w_up": noise(splits[9], (D, FF), D ** -0.5, 0.1875, ((1, 16),)),
        "w_down": noise(splits[10], (FF, D), FF ** -0.5, 0.09375, ((0, 16),)),
    }


def layer_norm(vectors, gain_vec):
    row_mean = lax.optimization_barrier(jnp.mean(vectors, axis=-1, keepdims=True))
    center = vectors - row_mean
    spread = lax.optimization_barrier(jnp.mean(center * center, axis=-1, keepdims=True))
    return center * lax.rsqrt(spread + 1e-06) * gain_vec.astype(jnp.float32)

def stem_image(pixels, stem_first, stem_conv):
    first_map = jnp.einsum('khw,kc->hwc', pixels.astype(jnp.float32), stem_first.astype(jnp.float32))
    stem_maps = jnp.maximum(first_map, 0.0).astype(jnp.bfloat16)
    padded = jnp.pad(stem_maps, ((1, 1), (1, 1), (0, 0)))
    height = stem_maps.shape[0]
    tile_width = stem_maps.shape[1]
    summed = stem_maps.astype(jnp.float32)
    for offset_a in range(3):
        for offset_b in range(3):
            window = padded[offset_a:offset_a + height, offset_b:offset_b + tile_width, :].astype(jnp.float32)
            summed = summed + jnp.einsum('hwc,cd->hwd', window, stem_conv[offset_a, offset_b].astype(jnp.float32))
    deep_maps = jnp.maximum(summed, 0.0).astype(jnp.bfloat16)
    blocks = deep_maps.reshape(height // 4, 4, tile_width // 4, 4, C).transpose(2, 0, 1, 3, 4)
    return blocks.reshape(height // 4 * (tile_width // 4), 16 * C)

def group_sum(left, right_side):
    group_width = left.shape[1] // N_COL
    left_groups = left.reshape(left.shape[0], N_COL, group_width).astype(jnp.float32)
    right_groups = right_side.reshape(N_COL, group_width, right_side.shape[1]).astype(jnp.float32)
    terms = jnp.einsum('tgh,ghd->gtd', left_groups, right_groups).astype(jnp.bfloat16)
    terms = lax.optimization_barrier(terms)
    return lax.optimization_barrier(jnp.sum(terms.astype(jnp.float32), axis=0))

def encoder_layer(embedded, gain_attn, w_qkv, w_out, gain_mlp, w_up, w_down):
    residual = embedded.astype(jnp.float32)
    normed = layer_norm(residual, gain_attn).astype(jnp.bfloat16)
    projected = jnp.einsum('td,kdh->kth', normed.astype(jnp.float32), w_qkv.astype(jnp.float32)).astype(jnp.bfloat16)
    token_count = embedded.shape[0]
    split_heads = projected.reshape(3, token_count, HEADS, HD).transpose(0, 2, 1, 3)

    def one_head(triple):
        queries, key_rows, value_rows = triple
        scores = jnp.einsum('qd,kd->qk', queries.astype(jnp.float32), key_rows.astype(jnp.float32)) * HD ** (-0.5)
        row_peak = lax.optimization_barrier(jnp.max(scores, axis=-1, keepdims=True))
        expo = jnp.exp(scores - row_peak)
        prob_rows = (expo / lax.optimization_barrier(jnp.sum(expo, axis=-1, keepdims=True))).astype(jnp.bfloat16)
        return jnp.einsum('qk,kd->qd', prob_rows.astype(jnp.float32), value_rows.astype(jnp.float32)).astype(jnp.bfloat16)
    attended = lax.map(one_head, (split_heads[0], split_heads[1], split_heads[2]))
    mixed_heads = attended.transpose(1, 0, 2).reshape(token_count, HEADS * HD)
    after = residual + group_sum(mixed_heads, w_out)
    normed_mlp = layer_norm(after, gain_mlp).astype(jnp.bfloat16)
    hidden = jax.nn.gelu(jnp.dot(normed_mlp, w_up, preferred_element_type=jnp.float32), approximate=True).astype(jnp.bfloat16)
    return (after + group_sum(hidden, w_down)).astype(jnp.bfloat16)

def reference(images, stem_first, stem_conv, patch_weight, position, gain_attn, w_qkv, w_out, gain_mlp, w_up, w_down):
    flat_images = images.reshape(MB * IMGS, 48, 4 * TROWS, 4 * TCOLS)
    position_rows = position.reshape(TCOLS * TROWS, D).astype(jnp.float32)

    def one_image(pixels):
        features = stem_image(pixels, stem_first, stem_conv)
        embedded = (jnp.dot(features, patch_weight, preferred_element_type=jnp.float32) + position_rows).astype(jnp.bfloat16)
        return encoder_layer(embedded, gain_attn, w_qkv, w_out, gain_mlp, w_up, w_down)
    results = lax.map(one_image, flat_images)
    results = results.reshape(MB, IMGS, TCOLS, TROWS, D)
    return jnp.roll(results, 1, axis=0)
```

```python
import math

import jax
import jax.numpy as jnp
from jax import lax
from jax.sharding import PartitionSpec as P

HD = 64
TEAM = 4


def layer_norm(vectors, gain_vec):
    row_mean = jnp.mean(vectors, axis=-1, keepdims=True)
    center = vectors - row_mean
    spread = jnp.mean(center * center, axis=-1, keepdims=True)
    return center * lax.rsqrt(spread + 1e-06) * gain_vec


def image_strip(images):
    sections = lax.axis_size("section")
    rows = lax.axis_size("row")
    pixels = images[0]
    img_count, colours, height, width = pixels.shape
    pixels = pixels.reshape(img_count, colours, height * width)
    target = (lax.axis_index("section") + 1) % sections
    slots = lax.broadcasted_iota(jnp.int32, (sections, 1, 1, 1), 0)
    outgoing = jnp.where(slots == target, pixels[None], jnp.zeros((), pixels.dtype))
    outgoing = outgoing.reshape(sections * rows, colours, height * width)
    incoming = lax.all_to_all(outgoing, ("section", "row"), 0, 0, tiled=True)
    source = (lax.axis_index("section") + sections - 1) % sections
    return lax.dynamic_slice_in_dim(incoming, source * rows, rows, 0)


def stem_features(strip, height, width, stem_first, stem_conv):
    parts, colours, _ = strip.shape
    total = parts * height
    channels = stem_first.shape[1]
    by_column = strip.reshape(parts, colours, height, width)
    left_col = by_column[:, :, :, 0].transpose(1, 0, 2).reshape(colours, total)
    right_col = by_column[:, :, :, width - 1].transpose(1, 0, 2).reshape(colours, total)
    count = lax.axis_size("col")
    forward = [(i, i + 1) for i in range(count - 1)]
    backward = [(target, source) for source, target in forward]
    low = lax.ppermute(right_col, "col", forward)
    high = lax.ppermute(left_col, "col", backward)

    def first_of(values, spec):
        result = jnp.einsum(spec, values, stem_first, preferred_element_type=jnp.float32)
        return jnp.maximum(result, 0.0).astype(jnp.bfloat16)

    stem_maps = first_of(strip, "rkp,kc->rpc").reshape(total, width, channels)
    low_map = first_of(low, "kh,kc->hc").reshape(total, 1, channels)
    high_map = first_of(high, "kh,kc->hc").reshape(total, 1, channels)
    padded = jnp.concatenate([low_map, stem_maps, high_map], axis=1)
    padded = jnp.pad(padded, ((1, 1), (0, 0), (0, 0)))
    summed = stem_maps.astype(jnp.float32)
    for offset_a in range(3):
        for offset_b in range(3):
            window = padded[offset_a : offset_a + total, offset_b : offset_b + width, :]
            summed = summed + jnp.einsum(
                "hwc,cd->hwd",
                window,
                stem_conv[offset_a, offset_b],
                preferred_element_type=jnp.float32,
            )
    deep_maps = jnp.maximum(summed, 0.0).astype(jnp.bfloat16)
    blocks = deep_maps.reshape(total // 4, 4, width // 4, 4, channels).transpose(2, 0, 1, 3, 4)
    return blocks.reshape(width // 4 * (total // 4), 16 * channels)


def team_pairs(step):
    return [(i, i ^ step) for i in range(lax.axis_size("row"))]


def attention(projected):
    _, token_count, width = projected.shape
    local_heads = width // HD
    split_heads = projected.reshape(3, token_count, local_heads, HD).transpose(0, 2, 1, 3)
    key_heads = split_heads[1]
    value_heads = split_heads[2]
    block_rows = math.gcd(token_count, 512)
    query_blocks = (
        split_heads[0]
        .reshape(local_heads, token_count // block_rows, block_rows, HD)
        .transpose(1, 0, 2, 3)
    )

    def attend(query_block):
        scores = jnp.einsum(
            "hqd,hkd->hqk", query_block, key_heads, preferred_element_type=jnp.float32
        ) * HD ** (-0.5)
        row_peak = jnp.max(scores, axis=-1, keepdims=True)
        expo = jnp.exp(scores - row_peak)
        prob_rows = (expo / jnp.sum(expo, axis=-1, keepdims=True)).astype(jnp.bfloat16)
        return jnp.einsum(
            "hqk,hkd->hqd", prob_rows, value_heads, preferred_element_type=jnp.float32
        ).astype(jnp.bfloat16)

    attended = lax.map(attend, query_blocks)
    return attended.transpose(0, 2, 1, 3).reshape(token_count, local_heads * HD)


def on_device(
    images,
    stem_first,
    stem_conv,
    patch_weight,
    position,
    gain_attn,
    w_qkv,
    w_out,
    gain_mlp,
    w_up,
    w_down,
):
    cols = lax.axis_size("col")
    member = lax.axis_index("row") % TEAM
    model_width = patch_weight.shape[1]
    hidden_here = w_down.shape[0] // TEAM
    full_patch = lax.all_gather(patch_weight, "col", axis=0, tiled=True)
    strip = image_strip(images)
    features = stem_features(strip, images.shape[3], images.shape[4], stem_first, stem_conv)
    place = lax.all_gather(position, "row", axis=1, tiled=True)
    cols_here = place.shape[0]
    tokens_in = (
        jnp.dot(features, full_patch, preferred_element_type=jnp.float32)
        + place.reshape(-1, model_width).astype(jnp.float32)
    ).astype(jnp.bfloat16)
    token_rows = tokens_in.shape[0]
    residual = tokens_in.astype(jnp.float32)
    normed = layer_norm(residual, gain_attn).astype(jnp.bfloat16)
    all_normed = lax.all_gather(normed, "col", axis=0, tiled=True)
    packed = jnp.concatenate(
        [
            w_out,
            lax.dynamic_slice_in_dim(w_up.T, member * hidden_here, hidden_here, 0),
            lax.dynamic_slice_in_dim(w_down, member * hidden_here, hidden_here, 0),
        ],
        axis=0,
    )
    packed, all_normed = lax.optimization_barrier((packed, all_normed))
    gathered = lax.all_gather(packed, "col", axis=0, tiled=False)
    head_rows = w_out.shape[0]
    full_out = gathered[:, :head_rows].reshape(-1, model_width)
    up_rows = gathered[:, head_rows : head_rows + hidden_here].reshape(-1, model_width)
    down_rows = gathered[:, head_rows + hidden_here :].reshape(-1, model_width)

    projected = jnp.einsum(
        "td,kdh->kth", all_normed, w_qkv, preferred_element_type=jnp.float32
    ).astype(jnp.bfloat16)
    mixed = attention(projected)
    heads_back = lax.all_to_all(mixed.reshape(cols, token_rows, -1), "col", 0, 0, tiled=True)
    mixed_heads = heads_back.transpose(1, 0, 2).reshape(token_rows, -1)
    after = residual + jnp.dot(mixed_heads, full_out, preferred_element_type=jnp.float32)
    normed_mlp = layer_norm(after, gain_mlp).astype(jnp.bfloat16)
    team_tokens = [normed_mlp]
    for step in range(1, TEAM):
        team_tokens.append(lax.ppermute(normed_mlp, "row", team_pairs(step)))
    stacked = jnp.concatenate(team_tokens, axis=0)
    hidden = jax.nn.gelu(
        jnp.einsum("td,hd->th", stacked, up_rows, preferred_element_type=jnp.float32),
        approximate=True,
    ).astype(jnp.bfloat16)
    terms = jnp.dot(hidden, down_rows, preferred_element_type=jnp.float32)
    terms = terms.reshape(TEAM, token_rows, model_width)
    encoded = after + terms[0]
    for step in range(1, TEAM):
        encoded = encoded + lax.ppermute(
            terms[step].astype(jnp.bfloat16), "row", team_pairs(step)
        ).astype(jnp.float32)
    return encoded.astype(jnp.bfloat16).reshape(1, 1, cols_here, -1, model_width)


def solution(mesh):
    placed = (
        P("section", None, None, "row", "col"),
        P(),
        P(),
        P("col", None),
        P("col", "row", None),
        P(),
        P(None, None, "col"),
        P("col", None),
        P(),
        P(None, "col"),
        P("col", None),
    )
    return jax.shard_map(
        on_device,
        mesh=mesh,
        in_specs=placed,
        out_specs=P("section", "row", "col", None, None),
        check_vma=False,
    )
```

```python
import jax
import jax.numpy as jnp
from jax import lax
from jax.sharding import PartitionSpec as P

HD = 64
TEAM = 4


def layer_norm(vectors, gain_vec):
    row_mean = jnp.mean(vectors, axis=-1, keepdims=True)
    center = vectors - row_mean
    spread = jnp.mean(center * center, axis=-1, keepdims=True)
    return center * lax.rsqrt(spread + 1e-06) * gain_vec


def image_strip(images, position):
    sections = lax.axis_size("section")
    rows = lax.axis_size("row")
    pixels = images[0]
    img_count, colours, height, width = pixels.shape
    tile = height * width
    cols_here, rows_here, model_width = position.shape
    pixels = pixels.reshape(img_count, colours, tile)
    place = position.reshape(-1, tile)
    slot_rows = max(colours, place.shape[0])
    pixels = jnp.pad(pixels, ((0, 0), (0, slot_rows - colours), (0, 0)))
    place = jnp.pad(place, ((0, slot_rows - place.shape[0]), (0, 0)))
    here = lax.axis_index("section")
    slots = lax.broadcasted_iota(jnp.int32, (sections, 1, 1, 1), 0)
    outgoing = jnp.where(slots == here, place[None, None], pixels[None])
    outgoing = outgoing.reshape(sections * rows, slot_rows, tile)
    incoming = lax.all_to_all(outgoing, ("section", "row"), 0, 0, tiled=True)
    other = (here + 1) % sections
    strip = lax.dynamic_slice_in_dim(incoming, other * rows, rows, 0)[:, :colours]
    place = lax.dynamic_slice_in_dim(incoming, here * rows, rows, 0)
    place = place[:, : position.size // tile].reshape(rows, cols_here, rows_here, model_width)
    place = place.transpose(1, 0, 2, 3).reshape(cols_here * rows * rows_here, model_width)
    return strip, place


def moved(value, step):
    count = lax.axis_size("col")
    return lax.ppermute(value, "col", [(i, (i + step) % count) for i in range(count)])


def core_swapped(value):
    return lax.ppermute(value, "col", [(i, i ^ 1) for i in range(lax.axis_size("col"))])


def ring_step(below, above, last):
    if last:
        half = below.shape[0] // 2
        return moved(below[:half], 2), moved(above[half:], -2)
    return moved(below, 2), moved(above, -2)


def ring(shard, join, pauses=()):
    steps = lax.axis_size("col") // 4
    pieces = [(True, shard), (False, core_swapped(shard))]
    below, above = shard, shard
    for step in range(1, steps + 1):
        below, above = ring_step(below, above, step == steps)
        if step <= len(pauses):
            below, above = pauses[step - 1](below, above)
        pair = jnp.concatenate([below, above], axis=0) if step == steps else join(below, above)
        pieces += [(True, pair), (False, core_swapped(pair))]
    return pieces


def arrival_offsets(chips):
    offsets = [0]
    for step in range(1, chips // 2):
        offsets += [chips - step, step]
    return offsets + [chips // 2]


def to_arrival(blocks):
    pairs = blocks.reshape(-1, 2, *blocks.shape[1:])
    chips = pairs.shape[0]
    place = lax.axis_index("col")
    doubled = jnp.concatenate([pairs, pairs], axis=0)
    rolled = lax.dynamic_slice_in_dim(doubled, place // 2, chips, 0)
    even = place % 2 == 0
    own = jnp.where(even, rolled[:, 0], rolled[:, 1])
    other = jnp.where(even, rolled[:, 1], rolled[:, 0])
    order = arrival_offsets(chips)
    return [own[i] for i in order], [other[i] for i in order]


def from_arrival(own, other):
    chips = len(own)
    order = arrival_offsets(chips)
    place = lax.axis_index("col")
    blocks = jnp.stack(
        [jnp.stack([part[order.index(i)] for i in range(chips)]) for part in (own, other)]
    )
    doubled = jnp.concatenate([blocks, blocks], axis=1)
    rolled = lax.dynamic_slice_in_dim(doubled, (chips - place // 2) % chips, chips, 1)
    even = place % 2 == 0
    first = jnp.where(even, rolled[0], rolled[1])
    second = jnp.where(even, rolled[1], rolled[0])
    return jnp.stack([first, second], axis=1).reshape(2 * chips, *own[0].shape)


def split_rows(pieces, size):
    found = {True: [], False: []}
    for same, piece in pieces:
        found[same] += [piece[i : i + size] for i in range(0, piece.shape[0], size)]
    return found[True], found[False]


def stem_features(strip, height, width, stem_first, stem_conv, pause):
    parts, colours, _ = strip.shape
    total = parts * height
    channels = stem_first.shape[1]
    by_column = strip.reshape(parts, colours, height, width)
    left_col = by_column[:, :, :, 0].transpose(1, 0, 2).reshape(colours, total)
    right_col = by_column[:, :, :, width - 1].transpose(1, 0, 2).reshape(colours, total)
    count = lax.axis_size("col")
    forward = [(i, i + 1) for i in range(count - 1)]
    backward = [(target, source) for source, target in forward]
    low = lax.ppermute(right_col, "col", forward)
    high = lax.ppermute(left_col, "col", backward)

    def first_of(values, spec):
        result = jnp.einsum(spec, values, stem_first, preferred_element_type=jnp.float32)
        return jnp.maximum(result, 0.0).astype(jnp.bfloat16)

    stem_maps = first_of(strip, "rkp,kc->rpc").reshape(total, width, channels)
    low_map = first_of(low, "kh,kc->hc").reshape(total, 1, channels)
    high_map = first_of(high, "kh,kc->hc").reshape(total, 1, channels)
    padded = jnp.concatenate([low_map, stem_maps, high_map], axis=1)
    padded = jnp.pad(padded, ((1, 1), (0, 0), (0, 0)))
    summed = stem_maps.astype(jnp.float32)
    for offset_a in range(3):
        for offset_b in range(3):
            window = padded[offset_a : offset_a + total, offset_b : offset_b + width, :]
            summed = summed + jnp.einsum(
                "hwc,cd->hwd",
                window,
                stem_conv[offset_a, offset_b],
                preferred_element_type=jnp.float32,
            )
        if offset_a == 0:
            summed = pause(summed)
    deep_maps = jnp.maximum(summed, 0.0).astype(jnp.bfloat16)
    blocks = deep_maps.reshape(total // 4, 4, width // 4, 4, channels).transpose(1, 3, 2, 0, 4)
    return blocks.reshape(16, width // 4 * (total // 4), channels)


def team_pairs(step):
    return [(i, i ^ step) for i in range(lax.axis_size("row"))]


def attend(query_block, keys, values):
    scores = jnp.einsum(
        "qd,kd->qk", query_block, keys, preferred_element_type=jnp.float32
    ) * HD ** (-0.5)
    row_peak = jnp.max(scores, axis=-1, keepdims=True)
    expo = jnp.exp(scores - row_peak)
    prob_rows = (expo / jnp.sum(expo, axis=-1, keepdims=True)).astype(jnp.bfloat16)
    return jnp.einsum(
        "qk,kd->qd", prob_rows, values, preferred_element_type=jnp.float32
    ).astype(jnp.bfloat16)


def on_device(
    images,
    stem_first,
    stem_conv,
    patch_weight,
    position,
    gain_attn,
    w_qkv,
    w_out,
    gain_mlp,
    w_up,
    w_down,
):
    cols = lax.axis_size("col")
    member = lax.axis_index("row") % TEAM
    patch_rows, model_width = patch_weight.shape
    head_rows = w_out.shape[0]
    hidden_here = w_down.shape[0] // TEAM
    shard = jnp.concatenate([patch_weight, w_out], axis=0)
    held = {}

    def after_first(below, above):
        strip, place = image_strip(images, position)
        below, above, held["strip"] = lax.optimization_barrier((below, above, strip))
        held["place"] = place
        return below, above

    def after_second(below, above):
        def pause(summed):
            summed, held["below"], held["above"] = lax.optimization_barrier((summed, below, above))
            return summed

        held["blocks"] = stem_features(
            held["strip"], images.shape[3], images.shape[4], stem_first, stem_conv, pause
        )
        return held["below"], held["above"]

    def join(below, above):
        return jnp.concatenate(
            [below[:patch_rows], above[:patch_rows], below[patch_rows:], above[patch_rows:]], axis=0
        )

    early = ring(shard, join, (after_first, after_second))
    cols_here = position.shape[0]
    own_blocks, other_blocks = to_arrival(held["blocks"])
    summed = held["place"].astype(jnp.float32)
    out_of = {True: [], False: []}
    for same, piece in early:
        blocks = own_blocks if same else other_blocks
        count = piece.shape[0] // shard.shape[0]
        block = jnp.concatenate(blocks[:count], axis=1)
        del blocks[:count]
        summed = summed + jnp.dot(
            block, piece[: count * patch_rows], preferred_element_type=jnp.float32
        )
        rest = piece[count * patch_rows :]
        out_of[same] += [rest[i * head_rows : (i + 1) * head_rows] for i in range(count)]
    tokens_in = summed.astype(jnp.bfloat16)
    token_rows = tokens_in.shape[0]
    full_out = from_arrival(out_of[True], out_of[False]).reshape(-1, model_width)

    residual = tokens_in.astype(jnp.float32)
    normed = layer_norm(residual, gain_attn).astype(jnp.bfloat16)
    local_width = w_qkv.shape[2]
    weight_qkv = w_qkv.transpose(1, 0, 2).reshape(model_width, 3 * local_width)
    def stack(below, above):
        return jnp.concatenate([below, above], axis=0)

    projected = jnp.concatenate(
        [
            jnp.dot(piece, weight_qkv, preferred_element_type=jnp.float32).astype(jnp.bfloat16)
            for _, piece in sorted(ring(normed, stack), key=lambda item: not item[0])
        ],
        axis=0,
    )
    packed = jnp.concatenate(
        [
            lax.dynamic_slice_in_dim(w_up.T, member * hidden_here, hidden_here, 0),
            lax.dynamic_slice_in_dim(w_down, member * hidden_here, hidden_here, 0),
        ],
        axis=0,
    )
    packed, projected = lax.optimization_barrier((packed, projected))
    late_own, late_other = split_rows(ring(packed, stack), 2 * hidden_here)
    up_rows = jnp.concatenate([rows[:hidden_here] for rows in late_own + late_other], axis=0)
    down_rows = jnp.concatenate([rows[hidden_here:] for rows in late_own + late_other], axis=0)

    queries, keys, values = (
        projected[:, i * local_width : (i + 1) * local_width] for i in range(3)
    )
    block_rows = queries.shape[0] // 4
    mixed = lax.map(
        lambda block: attend(block, keys, values), queries.reshape(4, block_rows, local_width)
    )
    mixed = mixed.reshape(2, cols // 2, token_rows, local_width)
    mixed = from_arrival(list(mixed[0]), list(mixed[1]))
    heads_back = lax.all_to_all(mixed, "col", 0, 0, tiled=True)
    mixed_heads = heads_back.transpose(1, 0, 2).reshape(token_rows, -1)
    after = residual + jnp.dot(mixed_heads, full_out, preferred_element_type=jnp.float32)
    normed_mlp = layer_norm(after, gain_mlp).astype(jnp.bfloat16)
    team_tokens = [normed_mlp]
    for step in range(1, TEAM):
        team_tokens.append(lax.ppermute(normed_mlp, "row", team_pairs(step)))
    stacked = jnp.concatenate(team_tokens, axis=0)
    hidden = jax.nn.gelu(
        jnp.einsum("td,hd->th", stacked, up_rows, preferred_element_type=jnp.float32),
        approximate=True,
    ).astype(jnp.bfloat16)
    terms = jnp.dot(hidden, down_rows, preferred_element_type=jnp.float32)
    terms = terms.reshape(TEAM, token_rows, model_width)
    encoded = after + terms[0]
    for step in range(1, TEAM):
        encoded = encoded + lax.ppermute(
            terms[step].astype(jnp.bfloat16), "row", team_pairs(step)
        ).astype(jnp.float32)
    return encoded.astype(jnp.bfloat16).reshape(1, 1, cols_here, -1, model_width)


def solution(mesh):
    placed = (
        P("section", None, None, "row", "col"),
        P(),
        P(),
        P("col", None),
        P("col", "row", None),
        P(),
        P(None, None, "col"),
        P("col", None),
        P(),
        P(None, "col"),
        P("col", None),
    )
    return jax.shard_map(
        on_device,
        mesh=mesh,
        in_specs=placed,
        out_specs=P("section", "row", "col", None, None),
        check_vma=False,
    )
```

```python
import functools

import jax
import jax.numpy as jnp
from jax import lax
from jax.experimental import pallas as pl
from jax.experimental.pallas import tpu as pltpu
from jax.sharding import PartitionSpec as P

HD = 64
TEAM = 4


def layer_norm(vectors, gain_vec):
    row_mean = jnp.mean(vectors, axis=-1, keepdims=True)
    center = vectors - row_mean
    spread = jnp.mean(center * center, axis=-1, keepdims=True)
    return center * lax.rsqrt(spread + 1e-06) * gain_vec


def image_strip(images, position):
    sections = lax.axis_size("section")
    rows = lax.axis_size("row")
    pixels = images[0]
    img_count, colours, height, width = pixels.shape
    tile = height * width
    cols_here, rows_here, model_width = position.shape
    pixels = pixels.reshape(img_count, colours, tile)
    place = position.reshape(-1, tile)
    slot_rows = max(colours, place.shape[0])
    pixels = jnp.pad(pixels, ((0, 0), (0, slot_rows - colours), (0, 0)))
    place = jnp.pad(place, ((0, slot_rows - place.shape[0]), (0, 0)))
    here = lax.axis_index("section")
    slots = lax.broadcasted_iota(jnp.int32, (sections, 1, 1, 1), 0)
    outgoing = jnp.where(slots == here, place[None, None], pixels[None])
    outgoing = outgoing.reshape(sections * rows, slot_rows, tile)
    incoming = lax.all_to_all(outgoing, ("section", "row"), 0, 0, tiled=True)
    other = (here + 1) % sections
    strip = lax.dynamic_slice_in_dim(incoming, other * rows, rows, 0)[:, :colours]
    place = lax.dynamic_slice_in_dim(incoming, here * rows, rows, 0)
    place = place[:, : position.size // tile].reshape(rows, cols_here, rows_here, model_width)
    place = place.transpose(1, 0, 2, 3).reshape(cols_here * rows * rows_here, model_width)
    return strip, place


def moved(value, step):
    count = lax.axis_size("col")
    return lax.ppermute(value, "col", [(i, (i + step) % count) for i in range(count)])


def core_swapped(value):
    return lax.ppermute(value, "col", [(i, i ^ 1) for i in range(lax.axis_size("col"))])


def ring(shard, early_work):
    chips = lax.axis_size("col") // 2
    steps = chips // 2
    pieces = [(True, 0, shard), (False, 0, core_swapped(shard))]
    below, above = shard, shard
    for step in range(1, steps):
        if step > 2:
            held = [rows for _, _, rows in pieces[-6:-4]]
            below, above, held = lax.optimization_barrier((below, above, held))
            for i, rows in zip((-6, -5), held, strict=True):
                pieces[i] = (*pieces[i][:2], rows)
        below, above = moved(below, 2), moved(above, -2)
        pieces += [
            (False, chips - step, core_swapped(below)),
            (False, step, core_swapped(above)),
            (True, chips - step, below),
            (True, step, above),
        ]
    done = early_work(pieces[:-4])
    below, above, done = lax.optimization_barrier((below, above, done))
    pieces[-1] = (True, steps - 1, above)
    last = moved(below, 2)
    pieces += [(True, steps, last), (False, steps, core_swapped(last))]
    return pieces, done, above


def stem_features(strip, height, width, stem_first, stem_conv):
    parts, colours, _ = strip.shape
    total = parts * height
    channels = stem_first.shape[1]
    by_column = strip.reshape(parts, colours, height, width)
    left_col = by_column[:, :, :, 0].transpose(1, 0, 2).reshape(colours, total)
    right_col = by_column[:, :, :, width - 1].transpose(1, 0, 2).reshape(colours, total)
    count = lax.axis_size("col")
    forward = [(i, i + 1) for i in range(count - 1)]
    backward = [(target, source) for source, target in forward]
    low = lax.ppermute(right_col, "col", forward)
    high = lax.ppermute(left_col, "col", backward)

    def first_of(values, spec):
        result = jnp.einsum(spec, values, stem_first, preferred_element_type=jnp.float32)
        return jnp.maximum(result, 0.0).astype(jnp.bfloat16)

    stem_maps = first_of(strip, "rkp,kc->rpc").reshape(total, width, channels)
    low_map = first_of(low, "kh,kc->hc").reshape(total, 1, channels)
    high_map = first_of(high, "kh,kc->hc").reshape(total, 1, channels)
    padded = jnp.concatenate([low_map, stem_maps, high_map], axis=1)
    padded = jnp.pad(padded, ((1, 1), (0, 0), (0, 0)))
    summed = stem_maps.astype(jnp.float32)
    for offset_a in range(3):
        for offset_b in range(3):
            window = padded[offset_a : offset_a + total, offset_b : offset_b + width, :]
            summed = summed + jnp.einsum(
                "hwc,cd->hwd",
                window,
                stem_conv[offset_a, offset_b],
                preferred_element_type=jnp.float32,
            )
    deep_maps = jnp.maximum(summed, 0.0).astype(jnp.bfloat16)
    blocks = deep_maps.reshape(total // 4, 4, width // 4, 4, channels).transpose(2, 0, 1, 3, 4)
    return blocks.reshape(width // 4 * (total // 4), 16 * channels)


def team_pairs(step):
    return [(i, i ^ step) for i in range(lax.axis_size("row"))]


def matmul_nt(left, right):
    return lax.dot_general(
        left, right, (((1,), (1,)), ((), ())), preferred_element_type=jnp.float32
    )


def project(rows, weight_ref):
    pair = jnp.concatenate([weight_ref[0], weight_ref[2]], axis=0)
    query_value = matmul_nt(rows, pair).astype(jnp.bfloat16)
    keys = matmul_nt(weight_ref[1], rows).astype(jnp.bfloat16)
    return query_value, keys


def project_body(weight_ref, *refs):
    *piece_refs, query_value_ref, key_ref = refs
    start = 0
    for piece_ref in piece_refs:
        count = piece_ref.shape[0]
        query_value, keys = project(piece_ref[...], weight_ref)
        query_value_ref[start : start + count] = query_value
        key_ref[:, start : start + count] = keys
        start += count


def attention_body(chips, tokens, early, late, place_ref, weight_ref, qv_ref, early_key_ref, *refs):
    *piece_refs, out_ref, all_ref, key_ref = refs
    place = place_ref[0]
    chip, core = place // 2, place % 2
    key_ref[HD:, :] = jnp.zeros((HD, key_ref.shape[1]), key_ref.dtype)

    def store(same, offset, query_value, keys):
        at = 2 * lax.rem(chip + offset, chips) + (core if same else 1 - core)
        at = pl.multiple_of(at * tokens, tokens)
        all_ref[pl.ds(at, tokens), :] = query_value
        key_ref[:HD, pl.ds(at, tokens)] = keys

    start = 0
    for same, offset in early:
        part = slice(start, start + tokens)
        store(same, offset, qv_ref[part, :], early_key_ref[:, part])
        start += tokens
    for (same, offset), piece_ref in zip(late, piece_refs, strict=True):
        store(same, offset, *project(piece_ref[...], weight_ref))

    block = 2 * tokens
    scale = HD ** (-0.5)

    def attend(step, carry):
        for i in range(2):
            at = pl.multiple_of((2 * step + i) * block, block)
            scores = jnp.dot(
                all_ref[pl.ds(at, block), :], key_ref[...], preferred_element_type=jnp.float32
            )
            peak = jnp.max(scores, axis=-1, keepdims=True)
            expo = jnp.exp((scores - peak) * scale)
            total = jnp.sum(expo, axis=-1, keepdims=True)
            probs = (expo * (1.0 / total)).astype(jnp.bfloat16)
            mixed = jnp.dot(probs, all_ref[...], preferred_element_type=jnp.float32)
            for j in range(2):
                out = mixed[j * tokens : (j + 1) * tokens, :].T[HD:, :]
                out_ref[2 * (2 * step + i) + j] = out.astype(jnp.bfloat16)
        return carry

    lax.fori_loop(0, all_ref.shape[0] // (2 * block), attend, 0)


def cost(flops):
    return pl.CostEstimate(flops=flops, bytes_accessed=flops // 256, transcendentals=0)


VMEM = pl.BlockSpec(memory_space=pltpu.VMEM)


def early_projection(weight, pieces):
    rows = sum(piece.shape[0] for _, _, piece in pieces)
    return pl.pallas_call(
        project_body,
        out_shape=(
            jax.ShapeDtypeStruct((rows, 2 * HD), jnp.bfloat16),
            jax.ShapeDtypeStruct((HD, rows), jnp.bfloat16),
        ),
        in_specs=[VMEM] * (1 + len(pieces)),
        out_specs=(VMEM, VMEM),
        compiler_params=pltpu.CompilerParams(vmem_limit_bytes=32 << 20),
        cost_estimate=cost(6 * rows * HD * weight.shape[2]),
    )(weight, *(piece for _, _, piece in pieces))


def attended_heads(normed, w_qkv):
    cols = lax.axis_size("col")
    weight = w_qkv.transpose(0, 2, 1)
    tokens = normed.shape[0]
    pieces, (query_value, keys), mark = ring(normed, functools.partial(early_projection, weight))
    count = cols - 6
    early, late = pieces[:count], pieces[count:]
    body = functools.partial(
        attention_body,
        cols // 2,
        tokens,
        [(same, offset) for same, offset, _ in early],
        [(same, offset) for same, offset, _ in late],
    )
    heads = pl.pallas_call(
        body,
        out_shape=jax.ShapeDtypeStruct((cols, HD, tokens), jnp.bfloat16),
        in_specs=[pl.BlockSpec(memory_space=pltpu.SMEM)] + [VMEM] * (3 + len(late)),
        out_specs=VMEM,
        scratch_shapes=[
            pltpu.VMEM((cols * tokens, 2 * HD), jnp.bfloat16),
            pltpu.VMEM((2 * HD, cols * tokens), jnp.bfloat16),
        ],
        compiler_params=pltpu.CompilerParams(vmem_limit_bytes=40 << 20),
        cost_estimate=cost(16 * HD * (cols * tokens) ** 2),
    )
    return heads(
        lax.axis_index("col").reshape(1), weight, query_value, keys, *(piece for _, _, piece in late)
    ), mark


def out_body(heads_ref, weight_ref, tokens_ref, gain_ref, after_ref, normed_ref):
    heads = heads_ref[...].astype(jnp.float32).T.astype(jnp.bfloat16)
    after = tokens_ref[...].astype(jnp.float32) + jnp.dot(
        heads, weight_ref[...], preferred_element_type=jnp.float32
    )
    after_ref[...] = after
    normed_ref[...] = layer_norm(after, gain_ref[...]).astype(jnp.bfloat16)


def out_projection(heads, full_out, tokens_in, gain):
    width = full_out.shape[1]
    return pl.pallas_call(
        out_body,
        out_shape=(
            jax.ShapeDtypeStruct(tokens_in.shape, jnp.float32),
            jax.ShapeDtypeStruct(tokens_in.shape, jnp.bfloat16),
        ),
        in_specs=[VMEM] * 4,
        out_specs=(VMEM, VMEM),
        compiler_params=pltpu.CompilerParams(vmem_limit_bytes=32 << 20),
        cost_estimate=cost(2 * tokens_in.shape[0] * width * width),
    )(heads, full_out, tokens_in, gain.reshape(1, width))


def mlp_body(first_ref, second_ref, up_ref, down_ref, out_first_ref, out_second_ref, rows_ref, sum_ref):
    step = pl.program_id(0)
    tokens = first_ref.shape[0]

    @pl.when(step == 0)
    def _():
        rows_ref[:tokens] = first_ref[...]
        rows_ref[tokens:] = second_ref[...]
        sum_ref[...] = jnp.zeros_like(sum_ref)

    width = rows_ref.shape[1]
    up = up_ref[...].reshape(-1, width)
    down = down_ref[...].reshape(-1, width)
    hidden = jax.nn.gelu(matmul_nt(rows_ref[...], up), approximate=True).astype(jnp.bfloat16)
    sum_ref[...] += jnp.dot(hidden, down, preferred_element_type=jnp.float32)

    @pl.when(step == pl.num_programs(0) - 1)
    def _():
        out_first_ref[...] = sum_ref[:tokens].astype(out_first_ref.dtype)
        out_second_ref[...] = sum_ref[tokens:].astype(out_second_ref.dtype)


def mlp_terms(first, second, gathered, first_type):
    cols, rows, width = gathered.shape
    units = rows // 2
    per_step = 4
    whole = pl.BlockSpec(memory_space=pltpu.VMEM)
    return pl.pallas_call(
        mlp_body,
        grid=(cols // per_step,),
        out_shape=(
            jax.ShapeDtypeStruct(first.shape, first_type),
            jax.ShapeDtypeStruct(first.shape, jnp.bfloat16),
        ),
        in_specs=[
            whole,
            whole,
            pl.BlockSpec((per_step, units, width), lambda i: (i, 0, 0)),
            pl.BlockSpec((per_step, units, width), lambda i: (i, 1, 0)),
        ],
        out_specs=(whole, whole),
        scratch_shapes=[
            pltpu.VMEM((2 * first.shape[0], width), jnp.bfloat16),
            pltpu.VMEM((2 * first.shape[0], width), jnp.float32),
        ],
        compiler_params=pltpu.CompilerParams(
            vmem_limit_bytes=32 << 20, dimension_semantics=("arbitrary",)
        ),
        cost_estimate=cost(8 * first.shape[0] * width * cols * units),
    )(first, second, gathered, gathered)


def on_device(
    images,
    stem_first,
    stem_conv,
    patch_weight,
    position,
    gain_attn,
    w_qkv,
    w_out,
    gain_mlp,
    w_up,
    w_down,
):
    member = lax.axis_index("row") % TEAM
    model_width = patch_weight.shape[1]
    hidden_here = w_down.shape[0] // TEAM
    full_patch = lax.all_gather(patch_weight, "col", axis=0, tiled=True)
    strip, place = image_strip(images, position)
    cols_here = position.shape[0]
    features = stem_features(strip, images.shape[3], images.shape[4], stem_first, stem_conv)
    w_out, full_patch, features = lax.optimization_barrier((w_out, full_patch, features))
    full_out = lax.all_gather(w_out, "col", axis=0, tiled=True)
    tokens_in = (
        jnp.dot(features, full_patch, preferred_element_type=jnp.float32)
        + place.astype(jnp.float32)
    ).astype(jnp.bfloat16)
    token_rows = tokens_in.shape[0]
    normed = layer_norm(tokens_in.astype(jnp.float32), gain_attn).astype(jnp.bfloat16)
    heads, mark = attended_heads(normed, w_qkv)
    packed = jnp.concatenate(
        [
            lax.dynamic_slice_in_dim(w_up.T, member * hidden_here, hidden_here, 0),
            lax.dynamic_slice_in_dim(w_down, member * hidden_here, hidden_here, 0),
        ],
        axis=0,
    )
    packed, mark = lax.optimization_barrier((packed, mark))
    gathered = lax.all_gather(packed, "col", axis=0, tiled=False)
    heads_back = lax.all_to_all(heads, "col", 0, 0, tiled=True)
    after, normed_mlp = out_projection(
        heads_back.reshape(-1, token_rows), full_out, tokens_in, gain_mlp
    )
    near, far, farthest = (lax.ppermute(normed_mlp, "row", team_pairs(i)) for i in (1, 2, 3))
    own_term, near_term = mlp_terms(normed_mlp, near, gathered, jnp.float32)
    near_back = lax.ppermute(near_term, "row", team_pairs(1))
    far, farthest, near_term = lax.optimization_barrier((far, farthest, near_term))
    far_term, farthest_term = mlp_terms(far, farthest, gathered, jnp.bfloat16)
    encoded = after + own_term + near_back.astype(jnp.float32)
    for step, term in ((2, far_term), (3, farthest_term)):
        encoded = encoded + lax.ppermute(term, "row", team_pairs(step)).astype(jnp.float32)
    return encoded.astype(jnp.bfloat16).reshape(1, 1, cols_here, -1, model_width)


def solution(mesh):
    placed = (
        P("section", None, None, "row", "col"),
        P(),
        P(),
        P("col", None),
        P("col", "row", None),
        P(),
        P(None, None, "col"),
        P("col", None),
        P(),
        P(None, "col"),
        P("col", None),
    )
    return jax.shard_map(
        on_device,
        mesh=mesh,
        in_specs=placed,
        out_specs=P("section", "row", "col", None, None),
        check_vma=False,
    )
```

```python
import functools

import jax
import jax.numpy as jnp
from jax import lax
from jax.experimental import pallas as pl
from jax.experimental.pallas import tpu as pltpu
from jax.sharding import PartitionSpec as P

HD = 64
TEAM = 4
PAIR = 2


def cost(flops):
    return pl.CostEstimate(flops=flops, bytes_accessed=flops // 256, transcendentals=0)


VMEM = pl.BlockSpec(memory_space=pltpu.VMEM)
HBM = pl.BlockSpec(memory_space=pltpu.HBM)


def layer_norm(vectors, gain_vec):
    row_mean = jnp.mean(vectors, axis=-1, keepdims=True)
    center = vectors - row_mean
    spread = jnp.mean(center * center, axis=-1, keepdims=True)
    return center * lax.rsqrt(spread + 1e-06) * gain_vec


def image_strips(images, position):
    sections = lax.axis_size("section")
    rows = lax.axis_size("row")
    pixels = images[0]
    img_count, colours, height, width = pixels.shape
    tile = height * width
    cols_here, rows_here, model_width = position.shape
    pixels = pixels.reshape(img_count // PAIR, 1, PAIR * colours, tile)
    pixels = jnp.broadcast_to(pixels, (img_count // PAIR, PAIR, PAIR * colours, tile))
    pixels = pixels.reshape(img_count, PAIR * colours, tile)
    place = position.reshape(cols_here * rows_here, model_width // tile, tile)
    place = place.transpose(1, 0, 2).reshape(-1, tile)
    place_rows = place.shape[0]
    slot_rows = PAIR * colours
    place = jnp.pad(place, ((0, slot_rows - place_rows), (0, 0)))
    here = lax.axis_index("section")
    slots = lax.broadcasted_iota(jnp.int32, (sections, 1, 1, 1), 0)
    outgoing = jnp.where(slots == here, place[None, None], pixels[None])
    outgoing = outgoing.reshape(sections * rows, slot_rows, tile)
    incoming = lax.all_to_all(outgoing, ("section", "row"), 0, 0, tiled=True)
    other = (here + 1) % sections
    strips = lax.dynamic_slice_in_dim(incoming, other * rows, rows, 0)
    strips = strips.reshape(rows, PAIR, colours, tile).transpose(1, 0, 2, 3)
    place = lax.dynamic_slice_in_dim(incoming, here * rows, rows, 0)
    half_rows = place_rows // PAIR
    member = lax.axis_index("row") % PAIR
    place = lax.dynamic_slice_in_dim(place, member * half_rows, half_rows, 1)
    place = place.reshape(rows, -1, cols_here, rows_here, tile).transpose(2, 0, 3, 1, 4)
    return strips, place.reshape(cols_here, rows * rows_here, -1)


def moved(value, step):
    count = lax.axis_size("col")
    return lax.ppermute(value, "col", [(i, (i + step) % count) for i in range(count)])


def core_swapped(value):
    return lax.ppermute(value, "col", [(i, i ^ 1) for i in range(lax.axis_size("col"))])


def ring(shard, early_work):
    chips = lax.axis_size("col") // 2
    steps = chips // 2
    pieces = [(True, 0, shard), (False, 0, core_swapped(shard))]
    below, above = shard, shard
    for step in range(1, steps):
        if step > 2:
            held = [rows for _, _, rows in pieces[-6:-4]]
            below, above, held = lax.optimization_barrier((below, above, held))
            for i, rows in zip((-6, -5), held, strict=True):
                pieces[i] = (*pieces[i][:2], rows)
        below, above = moved(below, 2), moved(above, -2)
        pieces += [
            (False, chips - step, core_swapped(below)),
            (False, step, core_swapped(above)),
            (True, chips - step, below),
            (True, step, above),
        ]
    done = early_work(pieces[:-4])
    below, above, done = lax.optimization_barrier((below, above, done))
    pieces[-1] = (True, steps - 1, above)
    last = moved(below, 2)
    pieces += [(True, steps, last), (False, steps, core_swapped(last))]
    return pieces, done, above


def stem_body(parts, *refs):
    first_refs, low_refs, high_refs = (refs[i * parts : (i + 1) * parts] for i in range(3))
    weight_ref, out_ref, planes_ref = refs[3 * parts :]
    images, pixels, lanes = first_refs[0].shape
    width = 16
    count = pixels // (4 * width)
    row = lax.broadcasted_iota(jnp.int32, (count, parts * lanes), 0)
    group = images * count

    def put(a, b, slot, image, values):
        at = pl.multiple_of(slot * group + image * count, count)
        planes_ref[a + 1, b, pl.ds(at, count), :] = values.astype(jnp.bfloat16)
        if a == 3:
            moved_down = jnp.where(row == 0, 0.0, pltpu.roll(values, 1, 0))
            planes_ref[0, b, pl.ds(at, count), :] = moved_down.astype(jnp.bfloat16)
        if a == 0:
            moved_up = jnp.where(row == count - 1, 0.0, pltpu.roll(values, count - 1, 0))
            planes_ref[5, b, pl.ds(at, count), :] = moved_up.astype(jnp.bfloat16)

    def strided(part_refs, image, start, stride):
        return jnp.concatenate(
            [ref[image, pl.ds(start, count, stride=stride), :] for ref in part_refs], axis=1
        )

    def build(column, carry):
        j, b = column // 4, column % 4
        for image in range(images):
            for a in range(4):
                put(a, b, j + 1, image, strided(first_refs, image, width * a + column, 4 * width))
        return carry

    lax.fori_loop(0, width, build, 0)
    for image in range(images):
        for a in range(4):
            put(a, 3, 0, image, strided(low_refs, image, a, 4))
            put(a, 0, width // 4 + 1, image, strided(high_refs, image, a, 4))

    rows = width // 4 * group
    channels = out_ref.shape[1] // 16

    def convolve(phase, carry):
        a, b = phase // 4, phase % 4
        summed = planes_ref[a + 1, b, group : group + rows, :].astype(jnp.float32)
        for tap_a in range(3):
            for tap_b in range(3):
                column = b + tap_b + 3
                at = pl.multiple_of((column // 4) * group, group)
                window = planes_ref[a + tap_a, column % 4, pl.ds(at, rows), :]
                summed = summed + jnp.dot(
                    window, weight_ref[tap_a, tap_b], preferred_element_type=jnp.float32
                )
        at = pl.multiple_of(phase * channels, channels)
        out_ref[:, pl.ds(at, channels)] = jnp.maximum(summed, 0.0).astype(jnp.bfloat16)
        return carry

    lax.fori_loop(0, 16, convolve, 0)


def stem_features(strips, height, width, stem_first, stem_conv):
    images, parts, colours, _ = strips.shape
    total = parts * height
    channels = stem_first.shape[1]
    by_column = strips.reshape(images, parts, colours, height, width)

    def column(at):
        return by_column[:, :, :, :, at].transpose(2, 0, 1, 3).reshape(colours, images * total)

    count = lax.axis_size("col")
    forward = [(i, i + 1) for i in range(count - 1)]
    backward = [(target, source) for source, target in forward]
    low = lax.ppermute(column(width - 1), "col", forward)
    high = lax.ppermute(column(0), "col", backward)

    lanes = 128
    starts = range(0, channels, lanes)

    def first_of(values, spec, start):
        result = jnp.einsum(
            spec, values, stem_first[:, start : start + lanes], preferred_element_type=jnp.float32
        )
        result = lax.reduce_precision(jnp.maximum(result, 0.0), 8, 7)
        return result.reshape(images, -1, lanes)

    firsts = [first_of(strips, "mrkp,kc->mrpc", start) for start in starts]
    lows, highs = ([first_of(side, "kh,kc->hc", start) for start in starts] for side in (low, high))
    tokens = images * total * width // 16
    return pl.pallas_call(
        functools.partial(stem_body, len(starts)),
        out_shape=jax.ShapeDtypeStruct((tokens, 16 * channels), jnp.bfloat16),
        in_specs=[VMEM] * (3 * len(starts) + 1),
        out_specs=VMEM,
        scratch_shapes=[
            pltpu.VMEM((6, 4, (width // 4 + 2) * images * total // 4, channels), jnp.bfloat16)
        ],
        compiler_params=pltpu.CompilerParams(vmem_limit_bytes=28 << 20),
        cost_estimate=cost(18 * images * total * width * channels**2),
    )(*firsts, *lows, *highs, stem_conv)


def team_pairs(step):
    return [(i, i ^ step) for i in range(lax.axis_size("row"))]


def matmul_nt(left, right):
    return lax.dot_general(
        left, right, (((1,), (1,)), ((), ())), preferred_element_type=jnp.float32
    )


def project(rows, weight_ref):
    pair = jnp.concatenate([weight_ref[0], weight_ref[2]], axis=0)
    query_value = matmul_nt(rows, pair).astype(jnp.bfloat16)
    keys = matmul_nt(weight_ref[1], rows).astype(jnp.bfloat16)
    return query_value, keys


def project_body(weight_ref, *refs):
    *piece_refs, query_value_ref, key_ref = refs
    start = 0
    for piece_ref in piece_refs:
        count = piece_ref.shape[0]
        query_value, keys = project(piece_ref[...], weight_ref)
        query_value_ref[start : start + count] = query_value
        key_ref[:, start : start + count] = keys
        start += count


def attention_body(chips, tokens, early, late, place_ref, weight_ref, qv_ref, early_key_ref, *refs):
    *piece_refs, out_ref, all_ref, key_ref = refs
    place = place_ref[0]
    chip, core = place // 2, place % 2
    key_ref[HD:, :] = jnp.zeros((HD, key_ref.shape[1]), key_ref.dtype)

    def store(same, offset, query_value, keys):
        at = 2 * lax.rem(chip + offset, chips) + (core if same else 1 - core)
        at = pl.multiple_of(at * tokens, tokens)
        all_ref[pl.ds(at, tokens), :] = query_value
        key_ref[:HD, pl.ds(at, tokens)] = keys

    start = 0
    for same, offset in early:
        part = slice(start, start + tokens)
        store(same, offset, qv_ref[part, :], early_key_ref[:, part])
        start += tokens
    for (same, offset), piece_ref in zip(late, piece_refs, strict=True):
        store(same, offset, *project(piece_ref[...], weight_ref))

    block = 2 * tokens
    scale = HD ** (-0.5)

    def attend(step, carry):
        for i in range(2):
            at = pl.multiple_of((2 * step + i) * block, block)
            scores = jnp.dot(
                all_ref[pl.ds(at, block), :], key_ref[...], preferred_element_type=jnp.float32
            )
            peak = jnp.max(scores, axis=-1, keepdims=True)
            expo = jnp.exp((scores - peak) * scale)
            total = jnp.sum(expo, axis=-1, keepdims=True)
            probs = (expo * (1.0 / total)).astype(jnp.bfloat16)
            mixed = jnp.dot(probs, all_ref[...], preferred_element_type=jnp.float32)
            for j in range(2):
                out = mixed[j * tokens : (j + 1) * tokens, :].T[HD:, :]
                out_ref[2 * (2 * step + i) + j] = out.astype(jnp.bfloat16)
        return carry

    lax.fori_loop(0, all_ref.shape[0] // (2 * block), attend, 0)


def early_projection(weight, pieces):
    rows = sum(piece.shape[0] for _, _, piece in pieces)
    return pl.pallas_call(
        project_body,
        out_shape=(
            jax.ShapeDtypeStruct((rows, 2 * HD), jnp.bfloat16),
            jax.ShapeDtypeStruct((HD, rows), jnp.bfloat16),
        ),
        in_specs=[VMEM] * (1 + len(pieces)),
        out_specs=(VMEM, VMEM),
        compiler_params=pltpu.CompilerParams(vmem_limit_bytes=16 << 20),
        cost_estimate=cost(6 * rows * HD * weight.shape[2]),
    )(weight, *(piece for _, _, piece in pieces))


def attended_heads(normed, w_qkv):
    cols = lax.axis_size("col")
    weight = w_qkv.transpose(0, 2, 1)
    tokens = normed.shape[0]
    pieces, (query_value, keys), mark = ring(normed, functools.partial(early_projection, weight))
    count = cols - 6
    early, late = pieces[:count], pieces[count:]
    body = functools.partial(
        attention_body,
        cols // 2,
        tokens,
        [(same, offset) for same, offset, _ in early],
        [(same, offset) for same, offset, _ in late],
    )
    heads = pl.pallas_call(
        body,
        out_shape=jax.ShapeDtypeStruct((cols, HD, tokens), jnp.bfloat16),
        in_specs=[pl.BlockSpec(memory_space=pltpu.SMEM)] + [VMEM] * (3 + len(late)),
        out_specs=VMEM,
        scratch_shapes=[
            pltpu.VMEM((cols * tokens, 2 * HD), jnp.bfloat16),
            pltpu.VMEM((2 * HD, cols * tokens), jnp.bfloat16),
        ],
        compiler_params=pltpu.CompilerParams(vmem_limit_bytes=24 << 20),
        cost_estimate=cost(16 * HD * (cols * tokens) ** 2),
    )
    return heads(
        lax.axis_index("col").reshape(1), weight, query_value, keys, *(piece for _, _, piece in late)
    ), mark


def embed_body(
    half_ref, features_ref, gathered_ref, place_ref, own_ref, other_ref, left_ref, weight_ref, sems
):
    groups, per_group, channels, width = weight_ref.shape
    span = per_group * channels
    copies = [
        (
            pltpu.make_async_copy(
                features_ref.at[:, pl.ds(i * span, span)], left_ref.at[i], sems.at[0, i]
            ),
            pltpu.make_async_copy(
                gathered_ref.at[pl.ds(i * per_group, per_group), pl.ds(0, channels), :],
                weight_ref.at[i],
                sems.at[1, i],
            ),
        )
        for i in range(groups)
    ]
    for pair in copies:
        for copy in pair:
            copy.start()
    summed = jnp.zeros((features_ref.shape[0], width), jnp.float32)
    for i, pair in enumerate(copies):
        for copy in pair:
            copy.wait()
        summed = summed + jnp.dot(
            left_ref[i],
            weight_ref[i].reshape(span, width),
            preferred_element_type=jnp.float32,
        )
    columns, count, _ = place_ref.shape
    first_half = half_ref[0] == 0
    for column in range(columns):
        place = place_ref[column].astype(jnp.float32)
        first, second = (
            summed[(PAIR * column + image) * count :][:count] + place for image in range(PAIR)
        )
        part = slice(column * count, (column + 1) * count)
        own_ref[part, :] = jnp.where(first_half, first, second).astype(jnp.bfloat16)
        other_ref[part, :] = jnp.where(first_half, second, first).astype(jnp.bfloat16)


def embed(half, features, gathered, place):
    cols, _, width = gathered.shape
    groups = 4
    channels = features.shape[1] // cols
    out = jax.ShapeDtypeStruct((features.shape[0] // PAIR, width), jnp.bfloat16)
    return pl.pallas_call(
        embed_body,
        out_shape=(out, out),
        in_specs=[pl.BlockSpec(memory_space=pltpu.SMEM), HBM, HBM, VMEM],
        out_specs=(VMEM, VMEM),
        scratch_shapes=[
            pltpu.VMEM((groups, features.shape[0], features.shape[1] // groups), jnp.bfloat16),
            pltpu.VMEM((groups, cols // groups, channels, width), jnp.bfloat16),
            pltpu.SemaphoreType.DMA((2, groups)),
        ],
        compiler_params=pltpu.CompilerParams(vmem_limit_bytes=20 << 20),
        cost_estimate=cost(2 * features.size * width),
    )(half.reshape(1), features, gathered, place)


def out_body(heads_ref, gathered_ref, tokens_ref, gain_ref, after_ref, normed_ref, weight_ref, sems):
    first = gathered_ref.shape[1] - PAIR * HD
    copies = [
        pltpu.make_async_copy(
            gathered_ref.at[:, pl.ds(first + i * HD, HD), :], weight_ref.at[i], sems.at[i]
        )
        for i in range(PAIR)
    ]
    for copy in copies:
        copy.start()
    heads = heads_ref[...].astype(jnp.float32).T.astype(jnp.bfloat16)
    sides = []
    for i, copy in enumerate(copies):
        copy.wait()
        weight = weight_ref[i].reshape(heads.shape[1], weight_ref.shape[-1])
        sides.append(jnp.dot(heads, weight, preferred_element_type=jnp.float32))
    after = tokens_ref[...].astype(jnp.float32) + jnp.concatenate(sides, axis=1)
    after_ref[...] = after
    normed_ref[...] = layer_norm(after, gain_ref[...]).astype(jnp.bfloat16)


def out_projection(heads, gathered, tokens_in, gain):
    cols, _, half_width = gathered.shape
    width = tokens_in.shape[1]
    return pl.pallas_call(
        out_body,
        out_shape=(
            jax.ShapeDtypeStruct(tokens_in.shape, jnp.float32),
            jax.ShapeDtypeStruct(tokens_in.shape, jnp.bfloat16),
        ),
        in_specs=[VMEM, HBM, VMEM, VMEM],
        out_specs=(VMEM, VMEM),
        scratch_shapes=[
            pltpu.VMEM((PAIR, cols, HD, half_width), jnp.bfloat16),
            pltpu.SemaphoreType.DMA((PAIR,)),
        ],
        compiler_params=pltpu.CompilerParams(vmem_limit_bytes=16 << 20),
        cost_estimate=cost(2 * tokens_in.shape[0] * width * width),
    )(heads, gathered, tokens_in, gain.reshape(1, width))


def mlp_body(first_ref, second_ref, gathered_ref, out_first_ref, out_second_ref, weight_ref, sems):
    groups, per_group, units, width = weight_ref.shape
    copies = [
        pltpu.make_async_copy(
            gathered_ref.at[pl.ds(i * per_group, per_group)], weight_ref.at[i], sems.at[i]
        )
        for i in range(groups)
    ]
    for copy in copies:
        copy.start()
    tokens = first_ref.shape[0]
    rows = jnp.concatenate([first_ref[...], second_ref[...]], axis=0)
    summed = jnp.zeros(rows.shape, jnp.float32)
    for i, copy in enumerate(copies):
        copy.wait()
        up = weight_ref[i, :, : units // 2, :].reshape(-1, width)
        down = weight_ref[i, :, units // 2 :, :].reshape(-1, width)
        hidden = jax.nn.gelu(matmul_nt(rows, up), approximate=True).astype(jnp.bfloat16)
        summed = summed + jnp.dot(hidden, down, preferred_element_type=jnp.float32)
    out_first_ref[...] = summed[:tokens].astype(out_first_ref.dtype)
    out_second_ref[...] = summed[tokens:].astype(out_second_ref.dtype)


def mlp_terms(first, second, gathered, first_type):
    cols, rows, width = gathered.shape
    groups = 4
    return pl.pallas_call(
        mlp_body,
        out_shape=(
            jax.ShapeDtypeStruct(first.shape, first_type),
            jax.ShapeDtypeStruct(first.shape, jnp.bfloat16),
        ),
        in_specs=[VMEM, VMEM, HBM],
        out_specs=(VMEM, VMEM),
        scratch_shapes=[
            pltpu.VMEM((groups, cols // groups, rows, width), jnp.bfloat16),
            pltpu.SemaphoreType.DMA((groups,)),
        ],
        compiler_params=pltpu.CompilerParams(vmem_limit_bytes=20 << 20),
        cost_estimate=cost(4 * first.shape[0] * width * cols * rows),
    )(first, second, gathered)


def on_device(
    images,
    stem_first,
    stem_conv,
    patch_weight,
    position,
    gain_attn,
    w_qkv,
    w_out,
    gain_mlp,
    w_up,
    w_down,
):
    member = lax.axis_index("row") % TEAM
    model_width = patch_weight.shape[1]
    hidden_here = w_down.shape[0] // TEAM
    half = lax.axis_index("row") % PAIR
    half_width = model_width // PAIR
    half_patch = lax.dynamic_slice_in_dim(patch_weight, half * half_width, half_width, 1)
    first_shard = jnp.concatenate(
        [half_patch, w_out[:, :half_width], w_out[:, half_width:]], axis=0
    )
    first_weights = lax.all_gather(first_shard, "col", axis=0, tiled=False)
    first_weights = pltpu.with_memory_space_constraint(first_weights, pltpu.HBM)
    strips, place = image_strips(images, position)
    packed = jnp.concatenate(
        [
            lax.dynamic_slice_in_dim(w_up.T, member * hidden_here, hidden_here, 0),
            lax.dynamic_slice_in_dim(w_down, member * hidden_here, hidden_here, 0),
        ],
        axis=0,
    )
    packed, strips = lax.optimization_barrier((packed, strips))
    cols_here = position.shape[0]
    features = stem_features(strips, images.shape[3], images.shape[4], stem_first, stem_conv)
    features = pltpu.with_memory_space_constraint(features, pltpu.HBM)
    even = half == 0
    own, others = embed(half, features, first_weights, place)
    others = lax.ppermute(others, "row", team_pairs(1))
    tokens_in = jnp.concatenate(
        [jnp.where(even, own, others), jnp.where(even, others, own)], axis=1
    )
    token_rows = tokens_in.shape[0]
    normed = layer_norm(tokens_in.astype(jnp.float32), gain_attn).astype(jnp.bfloat16)
    heads, mark = attended_heads(normed, w_qkv)
    packed, mark = lax.optimization_barrier((packed, mark))
    gathered = lax.all_gather(packed, "col", axis=0, tiled=False)
    gathered = pltpu.with_memory_space_constraint(gathered, pltpu.HBM)
    heads_back = lax.all_to_all(heads, "col", 0, 0, tiled=True)
    after, normed_mlp = out_projection(
        heads_back.reshape(-1, token_rows), first_weights, tokens_in, gain_mlp
    )
    near, far, farthest = (lax.ppermute(normed_mlp, "row", team_pairs(i)) for i in (1, 2, 3))
    own_term, near_term = mlp_terms(normed_mlp, near, gathered, jnp.float32)
    far, farthest, near_term = lax.optimization_barrier((far, farthest, near_term))
    near_back = lax.ppermute(near_term, "row", team_pairs(1))
    far_term, farthest_term = mlp_terms(far, farthest, gathered, jnp.bfloat16)
    encoded = after + own_term + near_back.astype(jnp.float32)
    for step, term in ((2, far_term), (3, farthest_term)):
        encoded = encoded + lax.ppermute(term, "row", team_pairs(step)).astype(jnp.float32)
    return encoded.astype(jnp.bfloat16).reshape(1, 1, cols_here, -1, model_width)


def solution(mesh):
    placed = (
        P("section", None, None, "row", "col"),
        P(),
        P(),
        P("col", None),
        P("col", "row", None),
        P(),
        P(None, None, "col"),
        P("col", None),
        P(),
        P(None, "col"),
        P("col", None),
    )
    return jax.shard_map(
        on_device,
        mesh=mesh,
        in_specs=placed,
        out_specs=P("section", "row", "col", None, None),
        check_vma=False,
    )
```

```python
import functools

import jax
import jax.numpy as jnp
from jax import lax
from jax.experimental import pallas as pl
from jax.experimental.pallas import tpu as pltpu
from jax.sharding import PartitionSpec as P

HD = 64
TEAM = 4
PAIR = 2


def cost(flops):
    return pl.CostEstimate(flops=flops, bytes_accessed=flops // 256, transcendentals=0)


VMEM = pl.BlockSpec(memory_space=pltpu.VMEM)
HBM = pl.BlockSpec(memory_space=pltpu.HBM)


def layer_norm(vectors, gain_vec):
    row_mean = jnp.mean(vectors, axis=-1, keepdims=True)
    center = vectors - row_mean
    spread = jnp.mean(center * center, axis=-1, keepdims=True)
    return center * lax.rsqrt(spread + 1e-06) * gain_vec


def image_strips(images, position):
    sections = lax.axis_size("section")
    rows = lax.axis_size("row")
    pixels = images[0]
    img_count, colours, height, width = pixels.shape
    tile = height * width
    cols_here, rows_here, model_width = position.shape
    pixels = pixels.reshape(img_count // PAIR, 1, PAIR * colours, tile)
    pixels = jnp.broadcast_to(pixels, (img_count // PAIR, PAIR, PAIR * colours, tile))
    pixels = pixels.reshape(img_count, PAIR * colours, tile)
    place = position.reshape(cols_here * rows_here, model_width // tile, tile)
    place = place.transpose(1, 0, 2).reshape(-1, tile)
    place_rows = place.shape[0]
    slot_rows = PAIR * colours
    place = jnp.pad(place, ((0, slot_rows - place_rows), (0, 0)))
    here = lax.axis_index("section")
    slots = lax.broadcasted_iota(jnp.int32, (sections, 1, 1, 1), 0)
    outgoing = jnp.where(slots == here, place[None, None], pixels[None])
    outgoing = outgoing.reshape(sections * rows, slot_rows, tile)
    incoming = lax.all_to_all(outgoing, ("section", "row"), 0, 0, tiled=True)
    other = (here + 1) % sections
    strips = lax.dynamic_slice_in_dim(incoming, other * rows, rows, 0)
    strips = strips.reshape(rows, PAIR, colours, tile).transpose(1, 0, 2, 3)
    place = lax.dynamic_slice_in_dim(incoming, here * rows, rows, 0)
    half_rows = place_rows // PAIR
    member = lax.axis_index("row") % PAIR
    place = lax.dynamic_slice_in_dim(place, member * half_rows, half_rows, 1)
    place = place.reshape(rows, -1, cols_here, rows_here, tile).transpose(2, 0, 3, 1, 4)
    return strips, place.reshape(cols_here, rows * rows_here, -1)


def moved(value, step):
    count = lax.axis_size("col")
    return lax.ppermute(value, "col", [(i, (i + step) % count) for i in range(count)])


def core_swapped(value):
    return lax.ppermute(value, "col", [(i, i ^ 1) for i in range(lax.axis_size("col"))])


def ring(shard, early_work):
    chips = lax.axis_size("col") // 2
    steps = chips // 2
    pieces = [(True, 0, shard), (False, 0, core_swapped(shard))]
    below, above = shard, shard
    for step in range(1, steps):
        if step > 2:
            below, above, first, second = lax.optimization_barrier(
                (below, above, pieces[-6][2], pieces[-5][2])
            )
            pieces[-6] = (*pieces[-6][:2], first)
            pieces[-5] = (*pieces[-5][:2], second)
        below, above = moved(below, 2), moved(above, -2)
        pieces += [
            (False, chips - step, core_swapped(below)),
            (False, step, core_swapped(above)),
            (True, chips - step, below),
            (True, step, above),
        ]
    done = early_work(pieces[:-4])
    below, above, done = lax.optimization_barrier((below, above, done))
    pieces[-1] = (True, steps - 1, above)
    last = moved(below, 2)
    pieces += [(True, steps, last), (False, steps, core_swapped(last))]
    return pieces, done, above


def stem_body(parts, *refs):
    first_refs = refs[:parts]
    low_ref, high_ref, first_weight_ref, conv_ref, out_ref = refs[parts : parts + 5]
    planes_ref, weight_ref, done_ref, low_refs, high_refs, sems = refs[parts + 5 :]
    images, pixels, lanes = first_refs[0].shape
    fetch = pltpu.make_async_copy(conv_ref, weight_ref, sems.at[16])
    fetch.start()
    low_refs = [low_refs.at[i] for i in range(parts)]
    high_refs = [high_refs.at[i] for i in range(parts)]
    for side_ref, side_refs in ((low_ref, low_refs), (high_ref, high_refs)):
        side = jnp.dot(
            side_ref[...].astype(jnp.float32).T.astype(jnp.bfloat16),
            first_weight_ref[...],
            preferred_element_type=jnp.float32,
        )
        side = jnp.maximum(side, 0.0).astype(jnp.bfloat16).astype(jnp.float32)
        for i, ref in enumerate(side_refs):
            ref[...] = side[:, i * lanes : (i + 1) * lanes].reshape(images, -1, lanes)
    width = 16
    count = pixels // (4 * width)
    row = lax.broadcasted_iota(jnp.int32, (count, parts * lanes), 0)
    group = images * count

    def put(a, b, slot, image, values):
        at = pl.multiple_of(slot * group + image * count, count)
        planes_ref[a + 1, b, pl.ds(at, count), :] = values.astype(jnp.bfloat16)
        if a == 3:
            moved_down = jnp.where(row == 0, 0.0, pltpu.roll(values, 1, 0))
            planes_ref[0, b, pl.ds(at, count), :] = moved_down.astype(jnp.bfloat16)
        if a == 0:
            moved_up = jnp.where(row == count - 1, 0.0, pltpu.roll(values, count - 1, 0))
            planes_ref[5, b, pl.ds(at, count), :] = moved_up.astype(jnp.bfloat16)

    def strided(part_refs, image, start, stride):
        return jnp.concatenate(
            [ref[image, pl.ds(start, count, stride=stride), :] for ref in part_refs], axis=1
        )

    def build(column, carry):
        j, b = column // 4, column % 4
        for image in range(images):
            for a in range(4):
                put(a, b, j + 1, image, strided(first_refs, image, width * a + column, 4 * width))
        return carry

    lax.fori_loop(0, width, build, 0)
    for image in range(images):
        for a in range(4):
            put(a, 3, 0, image, strided(low_refs, image, a, 4))
            put(a, 0, width // 4 + 1, image, strided(high_refs, image, a, 4))

    rows = width // 4 * group
    channels = out_ref.shape[1] // 16

    def sent(phase):
        at = pl.multiple_of(phase * channels, channels)
        return pltpu.make_async_copy(
            done_ref.at[phase], out_ref.at[:, pl.ds(at, channels)], sems.at[phase]
        )

    fetch.wait()

    def convolve(phase, carry):
        a, b = phase // 4, phase % 4
        summed = planes_ref[a + 1, b, group : group + rows, :].astype(jnp.float32)
        for tap_a in range(3):
            for tap_b in range(3):
                column = b + tap_b + 3
                at = pl.multiple_of((column // 4) * group, group)
                window = planes_ref[a + tap_a, column % 4, pl.ds(at, rows), :]
                summed = summed + jnp.dot(
                    window, weight_ref[tap_a, tap_b], preferred_element_type=jnp.float32
                )
        done_ref[phase] = jnp.maximum(summed, 0.0).astype(jnp.bfloat16)
        sent(phase).start()
        return carry

    lax.fori_loop(0, 16, convolve, 0)
    for phase in range(16):
        sent(phase).wait()


def stem_features(strips, height, width, stem_first, stem_conv):
    images, parts, colours, _ = strips.shape
    total = parts * height
    channels = stem_first.shape[1]
    by_column = strips.reshape(images, parts, colours, height, width)

    def column(at):
        return by_column[:, :, :, :, at].transpose(2, 0, 1, 3).reshape(colours, images * total)

    count = lax.axis_size("col")
    forward = [(i, i + 1) for i in range(count - 1)]
    backward = [(target, source) for source, target in forward]
    low = lax.ppermute(column(width - 1), "col", forward)
    high = lax.ppermute(column(0), "col", backward)

    lanes = 128
    starts = range(0, channels, lanes)

    def first_of(values, spec, start):
        result = jnp.einsum(
            spec, values, stem_first[:, start : start + lanes], preferred_element_type=jnp.float32
        )
        result = lax.reduce_precision(jnp.maximum(result, 0.0), 8, 7)
        return result.reshape(images, -1, lanes)

    firsts = [first_of(strips, "mrkp,kc->mrpc", start) for start in starts]
    tokens = images * total * width // 16
    return pl.pallas_call(
        functools.partial(stem_body, len(starts)),
        out_shape=pltpu.HBM((tokens, 16 * channels), jnp.bfloat16),
        in_specs=[VMEM] * (len(starts) + 3) + [HBM],
        out_specs=HBM,
        scratch_shapes=[
            pltpu.VMEM((6, 4, (width // 4 + 2) * images * total // 4, channels), jnp.bfloat16),
            pltpu.VMEM(stem_conv.shape, jnp.bfloat16),
            pltpu.VMEM((16, tokens, channels), jnp.bfloat16),
            pltpu.VMEM((len(starts), images, total, lanes), jnp.float32),
            pltpu.VMEM((len(starts), images, total, lanes), jnp.float32),
            pltpu.SemaphoreType.DMA((17,)),
        ],
        compiler_params=pltpu.CompilerParams(vmem_limit_bytes=20 << 20),
        cost_estimate=cost(18 * images * total * width * channels**2),
    )(
        *firsts,
        low,
        high,
        stem_first,
        pltpu.with_memory_space_constraint(stem_conv, pltpu.HBM),
    )


def team_pairs(step):
    return [(i, i ^ step) for i in range(lax.axis_size("row"))]


def matmul_nt(left, right):
    return lax.dot_general(
        left, right, (((1,), (1,)), ((), ())), preferred_element_type=jnp.float32
    )


def project(rows, weight_ref):
    pair = jnp.concatenate([weight_ref[0], weight_ref[2]], axis=0)
    query_value = matmul_nt(rows, pair).astype(jnp.bfloat16)
    keys = matmul_nt(weight_ref[1], rows).astype(jnp.bfloat16)
    return query_value, keys


def project_body(weight_ref, *refs):
    *piece_refs, query_value_ref, key_ref = refs
    start = 0
    for piece_ref in piece_refs:
        count = piece_ref.shape[0]
        query_value, keys = project(piece_ref[...], weight_ref)
        query_value_ref[start : start + count] = query_value
        key_ref[:, start : start + count] = keys
        start += count


def attention_body(chips, tokens, early, late, place_ref, weight_ref, qv_ref, early_key_ref, *refs):
    *piece_refs, out_ref, all_ref, key_ref, sems = refs
    place = place_ref[0]
    chip, core = place // 2, place % 2
    key_ref[HD:, :] = jnp.zeros((HD, key_ref.shape[1]), key_ref.dtype)

    def places(same, offset):
        at = 2 * lax.rem(chip + offset, chips) + (core if same else 1 - core)
        at = pl.ds(pl.multiple_of(at * tokens, tokens), tokens)
        return all_ref.at[at, :], key_ref.at[pl.ds(0, HD), at]

    copies = []
    for i, (same, offset) in enumerate(early):
        part = pl.ds(i * tokens, tokens)
        query_value, keys = places(same, offset)
        copies += [
            pltpu.make_async_copy(qv_ref.at[part, :], query_value, sems.at[0, i]),
            pltpu.make_async_copy(early_key_ref.at[:, part], keys, sems.at[1, i]),
        ]
    for copy in copies:
        copy.start()
    for (same, offset), piece_ref in zip(late, piece_refs, strict=True):
        for ref, values in zip(
            places(same, offset), project(piece_ref[...], weight_ref), strict=True
        ):
            ref[...] = values
    for copy in copies:
        copy.wait()

    block = 2 * tokens
    scale = HD ** (-0.5)

    def attend(step, carry):
        for i in range(2):
            at = pl.multiple_of((2 * step + i) * block, block)
            scores = jnp.dot(
                all_ref[pl.ds(at, block), :], key_ref[...], preferred_element_type=jnp.float32
            )
            peak = jnp.max(scores, axis=-1, keepdims=True)
            expo = jnp.exp((scores - peak) * scale)
            total = jnp.sum(expo, axis=-1, keepdims=True)
            probs = (expo * (1.0 / total)).astype(jnp.bfloat16)
            mixed = jnp.dot(probs, all_ref[...], preferred_element_type=jnp.float32)
            for j in range(2):
                out = mixed[j * tokens : (j + 1) * tokens, :].T[HD:, :]
                out_ref[2 * (2 * step + i) + j] = out.astype(jnp.bfloat16)
        return carry

    lax.fori_loop(0, all_ref.shape[0] // (2 * block), attend, 0)


def early_projection(weight, pieces):
    rows = sum(piece.shape[0] for _, _, piece in pieces)
    return pl.pallas_call(
        project_body,
        out_shape=(
            pltpu.HBM((rows, 2 * HD), jnp.bfloat16),
            pltpu.HBM((HD, rows), jnp.bfloat16),
        ),
        in_specs=[VMEM] * (1 + len(pieces)),
        out_specs=(VMEM, VMEM),
        compiler_params=pltpu.CompilerParams(vmem_limit_bytes=8 << 20),
        cost_estimate=cost(6 * rows * HD * weight.shape[2]),
    )(weight, *(piece for _, _, piece in pieces))


def attended_heads(normed, w_qkv):
    cols = lax.axis_size("col")
    weight = w_qkv.transpose(0, 2, 1)
    tokens = normed.shape[0]
    pieces, (query_value, keys), mark = ring(normed, functools.partial(early_projection, weight))
    count = cols - 6
    early, late = pieces[:count], pieces[count:]
    body = functools.partial(
        attention_body,
        cols // 2,
        tokens,
        [(same, offset) for same, offset, _ in early],
        [(same, offset) for same, offset, _ in late],
    )
    heads = pl.pallas_call(
        body,
        out_shape=jax.ShapeDtypeStruct((cols, HD, tokens), jnp.bfloat16),
        in_specs=[pl.BlockSpec(memory_space=pltpu.SMEM), VMEM, HBM, HBM] + [VMEM] * len(late),
        out_specs=VMEM,
        scratch_shapes=[
            pltpu.VMEM((cols * tokens, 2 * HD), jnp.bfloat16),
            pltpu.VMEM((2 * HD, cols * tokens), jnp.bfloat16),
            pltpu.SemaphoreType.DMA((2, len(early))),
        ],
        compiler_params=pltpu.CompilerParams(vmem_limit_bytes=14 << 20),
        cost_estimate=cost(16 * HD * (cols * tokens) ** 2),
    )
    return heads(
        lax.axis_index("col").reshape(1),
        weight,
        pltpu.with_memory_space_constraint(query_value, pltpu.HBM),
        pltpu.with_memory_space_constraint(keys, pltpu.HBM),
        *(piece for _, _, piece in late)
    ), mark


def embed_body(
    half_ref, features_ref, gathered_ref, place_ref, own_ref, other_ref, left_ref, weight_ref, sems
):
    groups, per_group, channels, width = weight_ref.shape
    span = per_group * channels
    copies = [
        (
            pltpu.make_async_copy(
                features_ref.at[:, pl.ds(i * span, span)], left_ref.at[i], sems.at[0, i]
            ),
            pltpu.make_async_copy(
                gathered_ref.at[pl.ds(i * per_group, per_group), pl.ds(0, channels), :],
                weight_ref.at[i],
                sems.at[1, i],
            ),
        )
        for i in range(groups)
    ]
    for pair in copies:
        for copy in pair:
            copy.start()
    summed = jnp.zeros((features_ref.shape[0], width), jnp.float32)
    for i, pair in enumerate(copies):
        for copy in pair:
            copy.wait()
        summed = summed + jnp.dot(
            left_ref[i],
            weight_ref[i].reshape(span, width),
            preferred_element_type=jnp.float32,
        )
    columns, count, _ = place_ref.shape
    first_half = half_ref[0] == 0
    for column in range(columns):
        place = place_ref[column].astype(jnp.float32)
        first, second = (
            summed[(PAIR * column + image) * count :][:count] + place for image in range(PAIR)
        )
        part = slice(column * count, (column + 1) * count)
        own_ref[part, :] = jnp.where(first_half, first, second).astype(jnp.bfloat16)
        other_ref[part, :] = jnp.where(first_half, second, first).astype(jnp.bfloat16)


def embed(half, features, gathered, place):
    cols, _, width = gathered.shape
    groups = 4
    channels = features.shape[1] // cols
    out = jax.ShapeDtypeStruct((features.shape[0] // PAIR, width), jnp.bfloat16)
    return pl.pallas_call(
        embed_body,
        out_shape=(out, out),
        in_specs=[pl.BlockSpec(memory_space=pltpu.SMEM), HBM, HBM, VMEM],
        out_specs=(VMEM, VMEM),
        scratch_shapes=[
            pltpu.VMEM((groups, features.shape[0], features.shape[1] // groups), jnp.bfloat16),
            pltpu.VMEM((groups, cols // groups, channels, width), jnp.bfloat16),
            pltpu.SemaphoreType.DMA((2, groups)),
        ],
        compiler_params=pltpu.CompilerParams(vmem_limit_bytes=20 << 20),
        cost_estimate=cost(2 * features.size * width),
    )(half.reshape(1), features, gathered, place)


def out_body(member_ref, heads_ref, *refs):
    *weight_refs, tokens_ref, gain_ref, after_ref, normed_ref = refs
    cols, rows, half_width = weight_refs[0].shape
    rows = rows // PAIR
    sides = [0.0] * PAIR
    for step, weight_ref in enumerate(weight_refs):
        at = pl.multiple_of(jnp.bitwise_xor(member_ref[0], step) * rows, rows)
        heads = heads_ref[:, pl.ds(at, rows), :].reshape(cols * rows, -1)
        heads = heads.astype(jnp.float32).T.astype(jnp.bfloat16)
        for i in range(PAIR):
            weight = weight_ref[:, i * rows : (i + 1) * rows, :].reshape(cols * rows, half_width)
            sides[i] = sides[i] + jnp.dot(heads, weight, preferred_element_type=jnp.float32)
    after = tokens_ref[...].astype(jnp.float32) + jnp.concatenate(sides, axis=1)
    after_ref[...] = after
    normed_ref[...] = layer_norm(after, gain_ref[...]).astype(jnp.bfloat16)


def out_projection(member, heads, quarters, tokens_in, gain):
    width = tokens_in.shape[1]
    return pl.pallas_call(
        out_body,
        out_shape=(
            jax.ShapeDtypeStruct(tokens_in.shape, jnp.float32),
            jax.ShapeDtypeStruct(tokens_in.shape, jnp.bfloat16),
        ),
        in_specs=[pl.BlockSpec(memory_space=pltpu.SMEM)] + [VMEM] * (3 + len(quarters)),
        out_specs=(VMEM, VMEM),
        compiler_params=pltpu.CompilerParams(vmem_limit_bytes=10 << 20),
        cost_estimate=cost(2 * tokens_in.shape[0] * width * width),
    )(member.reshape(1), heads, *quarters, tokens_in, gain.reshape(1, width))


def mlp_body(first_ref, second_ref, gathered_ref, out_first_ref, out_second_ref, weight_ref, sems):
    groups, per_group, units, width = weight_ref.shape
    copies = [
        pltpu.make_async_copy(
            gathered_ref.at[pl.ds(i * per_group, per_group)], weight_ref.at[i], sems.at[i]
        )
        for i in range(groups)
    ]
    for copy in copies:
        copy.start()
    tokens = first_ref.shape[0]
    rows = jnp.concatenate([first_ref[...], second_ref[...]], axis=0)
    summed = jnp.zeros(rows.shape, jnp.float32)
    for i, copy in enumerate(copies):
        copy.wait()
        up = weight_ref[i, :, : units // 2, :].reshape(-1, width)
        down = weight_ref[i, :, units // 2 :, :].reshape(-1, width)
        hidden = jax.nn.gelu(matmul_nt(rows, up), approximate=True).astype(jnp.bfloat16)
        summed = summed + jnp.dot(hidden, down, preferred_element_type=jnp.float32)
    out_first_ref[...] = summed[:tokens].astype(out_first_ref.dtype)
    out_second_ref[...] = summed[tokens:].astype(out_second_ref.dtype)


def mlp_terms(first, second, gathered, first_type):
    cols, rows, width = gathered.shape
    groups = 4
    return pl.pallas_call(
        mlp_body,
        out_shape=(
            jax.ShapeDtypeStruct(first.shape, first_type),
            jax.ShapeDtypeStruct(first.shape, jnp.bfloat16),
        ),
        in_specs=[VMEM, VMEM, HBM],
        out_specs=(VMEM, VMEM),
        scratch_shapes=[
            pltpu.VMEM((groups, cols // groups, rows, width), jnp.bfloat16),
            pltpu.SemaphoreType.DMA((groups,)),
        ],
        compiler_params=pltpu.CompilerParams(vmem_limit_bytes=20 << 20),
        cost_estimate=cost(4 * first.shape[0] * width * cols * rows),
    )(first, second, gathered)


def on_device(
    images,
    stem_first,
    stem_conv,
    patch_weight,
    position,
    gain_attn,
    w_qkv,
    w_out,
    gain_mlp,
    w_up,
    w_down,
):
    member = lax.axis_index("row") % TEAM
    model_width = patch_weight.shape[1]
    hidden_here = w_down.shape[0] // TEAM
    half = lax.axis_index("row") % PAIR
    half_width = model_width // PAIR
    half_patch = lax.dynamic_slice_in_dim(patch_weight, half * half_width, half_width, 1)
    out_here = w_out.shape[0] // TEAM
    out_quarter = lax.dynamic_slice_in_dim(w_out, member * out_here, out_here, 0)
    first_shard = jnp.concatenate(
        [half_patch, out_quarter[:, :half_width], out_quarter[:, half_width:]], axis=0
    )
    first_weights = lax.all_gather(first_shard, "col", axis=0, tiled=False)
    strips, place = image_strips(images, position)
    packed = jnp.concatenate(
        [
            lax.dynamic_slice_in_dim(w_up.T, member * hidden_here, hidden_here, 0),
            lax.dynamic_slice_in_dim(w_down, member * hidden_here, hidden_here, 0),
        ],
        axis=0,
    )
    packed, strips = lax.optimization_barrier((packed, strips))
    cols_here = position.shape[0]
    features = stem_features(strips, images.shape[3], images.shape[4], stem_first, stem_conv)
    even = half == 0
    own, others = embed(
        half,
        pltpu.with_memory_space_constraint(features, pltpu.HBM),
        pltpu.with_memory_space_constraint(first_weights, pltpu.HBM),
        place,
    )
    others = lax.ppermute(others, "row", team_pairs(1))
    tokens_in = jnp.concatenate(
        [jnp.where(even, own, others), jnp.where(even, others, own)], axis=1
    )
    quarter = first_weights[:, half_patch.shape[0] :]
    quarter, tokens_in = lax.optimization_barrier((quarter, tokens_in))
    quarters = [quarter]
    for step in range(1, TEAM):
        quarters.append(lax.ppermute(quarter, "row", team_pairs(step)))
    normed = layer_norm(tokens_in.astype(jnp.float32), gain_attn).astype(jnp.bfloat16)
    heads, mark = attended_heads(normed, w_qkv)
    packed, mark = lax.optimization_barrier((packed, mark))
    gathered = lax.all_gather(packed, "col", axis=0, tiled=False)
    gathered = pltpu.with_memory_space_constraint(gathered, pltpu.HBM)
    heads_back = lax.all_to_all(heads, "col", 0, 0, tiled=True)
    after, normed_mlp = out_projection(
        member, heads_back, quarters, tokens_in, gain_mlp
    )
    near, far, farthest = (lax.ppermute(normed_mlp, "row", team_pairs(i)) for i in (1, 2, 3))
    own_term, near_term = mlp_terms(normed_mlp, near, gathered, jnp.float32)
    far, farthest, near_term = lax.optimization_barrier((far, farthest, near_term))
    near_back = lax.ppermute(near_term, "row", team_pairs(1))
    far_term, farthest_term = mlp_terms(far, farthest, gathered, jnp.bfloat16)
    encoded = after + own_term + near_back.astype(jnp.float32)
    for step, term in ((2, far_term), (3, farthest_term)):
        encoded = encoded + lax.ppermute(term, "row", team_pairs(step)).astype(jnp.float32)
    return encoded.astype(jnp.bfloat16).reshape(1, 1, cols_here, -1, model_width)


def solution(mesh):
    placed = (
        P("section", None, None, "row", "col"),
        P(),
        P(),
        P("col", None),
        P("col", "row", None),
        P(),
        P(None, None, "col"),
        P("col", None),
        P(),
        P(None, "col"),
        P("col", None),
    )
    return jax.shard_map(
        on_device,
        mesh=mesh,
        in_specs=placed,
        out_specs=P("section", "row", "col", None, None),
        check_vma=False,
    )
```

```python
import functools
import math

import jax
import jax.numpy as jnp
from jax import lax
from jax.experimental import pallas as pl
from jax.experimental.pallas import tpu as pltpu
from jax.sharding import PartitionSpec as P

HD = 64
TEAM = 4
PAIR = 2


def cost(flops):
    return pl.CostEstimate(flops=flops, bytes_accessed=flops // 256, transcendentals=0)


VMEM = pl.BlockSpec(memory_space=pltpu.VMEM)
HBM = pl.BlockSpec(memory_space=pltpu.HBM)


def layer_norm(vectors, gain_vec):
    row_mean = jnp.mean(vectors, axis=-1, keepdims=True)
    center = vectors - row_mean
    spread = jnp.mean(center * center, axis=-1, keepdims=True)
    return center * lax.rsqrt(spread + 1e-06) * gain_vec


def image_strips(images, position):
    sections = lax.axis_size("section")
    rows = lax.axis_size("row")
    pixels = images[0]
    img_count, colours, height, width = pixels.shape
    tile = height * width
    cols_here, rows_here, model_width = position.shape
    pixels = pixels.reshape(img_count // PAIR, 1, PAIR * colours, tile)
    pixels = jnp.broadcast_to(pixels, (img_count // PAIR, PAIR, PAIR * colours, tile))
    pixels = pixels.reshape(img_count, PAIR * colours, tile)
    place = position.reshape(cols_here * rows_here, model_width // tile, tile)
    place = place.transpose(1, 0, 2).reshape(-1, tile)
    place_rows = place.shape[0]
    slot_rows = PAIR * colours
    place = jnp.pad(place, ((0, slot_rows - place_rows), (0, 0)))
    here = lax.axis_index("section")
    slots = lax.broadcasted_iota(jnp.int32, (sections, 1, 1, 1), 0)
    outgoing = jnp.where(slots == here, place[None, None], pixels[None])
    outgoing = outgoing.reshape(sections * rows, slot_rows, tile)
    incoming = lax.all_to_all(outgoing, ("section", "row"), 0, 0, tiled=True)
    other = (here + 1) % sections
    strips = lax.dynamic_slice_in_dim(incoming, other * rows, rows, 0)
    strips = strips.reshape(rows, PAIR, colours, tile).transpose(1, 0, 2, 3)
    place = lax.dynamic_slice_in_dim(incoming, here * rows, rows, 0)
    half_rows = place_rows // PAIR
    member = lax.axis_index("row") % PAIR
    place = lax.dynamic_slice_in_dim(place, member * half_rows, half_rows, 1)
    place = place.reshape(rows, -1, cols_here, rows_here, tile).transpose(2, 0, 3, 1, 4)
    return strips, place.reshape(cols_here, rows * rows_here, -1)


def moved(value, step):
    count = lax.axis_size("col")
    return lax.ppermute(value, "col", [(i, (i + step) % count) for i in range(count)])


def core_swapped(value):
    return lax.ppermute(value, "col", [(i, i ^ 1) for i in range(lax.axis_size("col"))])


def ring(shard, early_work):
    chips = lax.axis_size("col") // 2
    steps = chips // 2
    pieces = [(True, 0, shard), (False, 0, core_swapped(shard))]
    below, above = shard, shard
    for step in range(1, steps):
        if step > 2:
            below, above, first, second = lax.optimization_barrier(
                (below, above, pieces[-6][2], pieces[-5][2])
            )
            pieces[-6] = (*pieces[-6][:2], first)
            pieces[-5] = (*pieces[-5][:2], second)
        below, above = moved(below, 2), moved(above, -2)
        pieces += [
            (False, chips - step, core_swapped(below)),
            (False, step, core_swapped(above)),
            (True, chips - step, below),
            (True, step, above),
        ]
    done = early_work(pieces[:-4])
    below, above, done = lax.optimization_barrier((below, above, done))
    pieces[-1] = (True, steps - 1, above)
    count = lax.axis_size("col")
    last = lax.ppermute(
        jnp.where(lax.axis_index("col") % 2 == 0, below, above),
        "col",
        [(i, (i + (2 if i % 2 == 0 else -2)) % count) for i in range(count)],
    )
    pieces += [(True, steps, last), (False, steps, core_swapped(last))]
    return pieces, done, above


def stem_body(parts, *refs):
    first_refs = refs[:parts]
    low_ref, high_ref, first_weight_ref, conv_ref, out_ref = refs[parts : parts + 5]
    planes_ref, weight_ref, done_ref, low_refs, high_refs, sems = refs[parts + 5 :]
    images, pixels, lanes = first_refs[0].shape
    fetch = pltpu.make_async_copy(conv_ref, weight_ref, sems.at[16])
    fetch.start()
    low_refs = [low_refs.at[i] for i in range(parts)]
    high_refs = [high_refs.at[i] for i in range(parts)]
    for side_ref, side_refs in ((low_ref, low_refs), (high_ref, high_refs)):
        side = jnp.dot(
            side_ref[...].astype(jnp.float32).T.astype(jnp.bfloat16),
            first_weight_ref[...],
            preferred_element_type=jnp.float32,
        )
        side = jnp.maximum(side, 0.0).astype(jnp.bfloat16).astype(jnp.float32)
        for i, ref in enumerate(side_refs):
            ref[...] = side[:, i * lanes : (i + 1) * lanes].reshape(images, -1, lanes)
    width = 16
    count = pixels // (4 * width)
    row = lax.broadcasted_iota(jnp.int32, (count, parts * lanes), 0)
    group = images * count

    def put(a, b, slot, image, values):
        at = pl.multiple_of(slot * group + image * count, count)
        planes_ref[a + 1, b, pl.ds(at, count), :] = values.astype(jnp.bfloat16)
        if a == 3:
            moved_down = jnp.where(row == 0, 0.0, pltpu.roll(values, 1, 0))
            planes_ref[0, b, pl.ds(at, count), :] = moved_down.astype(jnp.bfloat16)
        if a == 0:
            moved_up = jnp.where(row == count - 1, 0.0, pltpu.roll(values, count - 1, 0))
            planes_ref[5, b, pl.ds(at, count), :] = moved_up.astype(jnp.bfloat16)

    def strided(part_refs, image, start, stride):
        return jnp.concatenate(
            [ref[image, pl.ds(start, count, stride=stride), :] for ref in part_refs], axis=1
        )

    def build(column, carry):
        j, b = column // 4, column % 4
        for image in range(images):
            for a in range(4):
                put(a, b, j + 1, image, strided(first_refs, image, width * a + column, 4 * width))
        return carry

    lax.fori_loop(0, width, build, 0)
    for image in range(images):
        for a in range(4):
            put(a, 3, 0, image, strided(low_refs, image, a, 4))
            put(a, 0, width // 4 + 1, image, strided(high_refs, image, a, 4))

    rows = width // 4 * group
    channels = out_ref.shape[1] // 16

    def sent(phase):
        at = pl.multiple_of(phase * channels, channels)
        return pltpu.make_async_copy(
            done_ref.at[phase], out_ref.at[:, pl.ds(at, channels)], sems.at[phase]
        )

    fetch.wait()

    def convolve(phase, carry):
        a, b = phase // 4, phase % 4
        summed = planes_ref[a + 1, b, group : group + rows, :].astype(jnp.float32)
        for tap_a in range(3):
            for tap_b in range(3):
                column = b + tap_b + 3
                at = pl.multiple_of((column // 4) * group, group)
                window = planes_ref[a + tap_a, column % 4, pl.ds(at, rows), :]
                summed = summed + jnp.dot(
                    window, weight_ref[tap_a, tap_b], preferred_element_type=jnp.float32
                )
        done_ref[phase] = jnp.maximum(summed, 0.0).astype(jnp.bfloat16)
        sent(phase).start()
        return carry

    lax.fori_loop(0, 16, convolve, 0)
    for phase in range(16):
        sent(phase).wait()


def stem_features(strips, height, width, stem_first, stem_conv):
    images, parts, colours, _ = strips.shape
    total = parts * height
    channels = stem_first.shape[1]
    by_column = strips.reshape(images, parts, colours, height, width)

    def column(at):
        return by_column[:, :, :, :, at].transpose(2, 0, 1, 3).reshape(colours, images * total)

    count = lax.axis_size("col")
    forward = [(i, i + 1) for i in range(count - 1)]
    backward = [(target, source) for source, target in forward]
    low = lax.ppermute(column(width - 1), "col", forward)
    high = lax.ppermute(column(0), "col", backward)

    lanes = 128
    starts = range(0, channels, lanes)

    def first_of(values, spec, start):
        result = jnp.einsum(
            spec, values, stem_first[:, start : start + lanes], preferred_element_type=jnp.float32
        )
        result = lax.reduce_precision(jnp.maximum(result, 0.0), 8, 7)
        return result.reshape(images, -1, lanes)

    firsts = [first_of(strips, "mrkp,kc->mrpc", start) for start in starts]
    tokens = images * total * width // 16
    return pl.pallas_call(
        functools.partial(stem_body, len(starts)),
        out_shape=pltpu.HBM((tokens, 16 * channels), jnp.bfloat16),
        in_specs=[VMEM] * (len(starts) + 3) + [HBM],
        out_specs=HBM,
        scratch_shapes=[
            pltpu.VMEM((6, 4, (width // 4 + 2) * images * total // 4, channels), jnp.bfloat16),
            pltpu.VMEM(stem_conv.shape, jnp.bfloat16),
            pltpu.VMEM((16, tokens, channels), jnp.bfloat16),
            pltpu.VMEM((len(starts), images, total, lanes), jnp.float32),
            pltpu.VMEM((len(starts), images, total, lanes), jnp.float32),
            pltpu.SemaphoreType.DMA((17,)),
        ],
        compiler_params=pltpu.CompilerParams(vmem_limit_bytes=20 << 20),
        cost_estimate=cost(18 * images * total * width * channels**2),
    )(
        *firsts,
        low,
        high,
        stem_first,
        pltpu.with_memory_space_constraint(stem_conv, pltpu.HBM),
    )


def team_pairs(step):
    return [(i, i ^ step) for i in range(lax.axis_size("row"))]


def matmul_nt(left, right):
    return lax.dot_general(
        left, right, (((1,), (1,)), ((), ())), preferred_element_type=jnp.float32
    )


def project(rows, weight_ref):
    pair = jnp.concatenate([weight_ref[0], weight_ref[2]], axis=0)
    query_value = matmul_nt(rows, pair).astype(jnp.bfloat16)
    keys = matmul_nt(weight_ref[1], rows).astype(jnp.bfloat16)
    return query_value, keys


def project_body(weight_ref, *refs):
    *piece_refs, query_value_ref, key_ref = refs
    start = 0
    for piece_ref in piece_refs:
        count = piece_ref.shape[0]
        query_value, keys = project(piece_ref[...], weight_ref)
        query_value_ref[start : start + count] = query_value
        key_ref[:, start : start + count] = keys
        start += count


def attention_body(chips, tokens, early, late, place_ref, weight_ref, qv_ref, early_key_ref, *refs):
    *piece_refs, out_ref, all_ref, key_ref, sems = refs
    place = place_ref[0]
    chip, core = place // 2, place % 2
    key_ref[HD:, :] = jnp.zeros((HD, key_ref.shape[1]), key_ref.dtype)

    def places(same, offset):
        at = 2 * lax.rem(chip + offset, chips) + (core if same else 1 - core)
        at = pl.ds(pl.multiple_of(at * tokens, tokens), tokens)
        return all_ref.at[at, :], key_ref.at[pl.ds(0, HD), at]

    copies = []
    for i, (same, offset) in enumerate(early):
        part = pl.ds(i * tokens, tokens)
        query_value, keys = places(same, offset)
        copies += [
            pltpu.make_async_copy(qv_ref.at[part, :], query_value, sems.at[0, i]),
            pltpu.make_async_copy(early_key_ref.at[:, part], keys, sems.at[1, i]),
        ]
    for copy in copies:
        copy.start()
    for (same, offset), piece_ref in zip(late, piece_refs, strict=True):
        for ref, values in zip(
            places(same, offset), project(piece_ref[...], weight_ref), strict=True
        ):
            ref[...] = values
    for copy in copies:
        copy.wait()

    block = 2 * tokens
    scale = HD ** (-0.5) * math.log2(math.e)

    def attend(step, carry):
        for i in range(2):
            at = pl.multiple_of((2 * step + i) * block, block)
            scores = jnp.dot(
                all_ref[pl.ds(at, block), :], key_ref[...], preferred_element_type=jnp.float32
            )
            peak = jnp.max(scores, axis=-1, keepdims=True)
            expo = jnp.exp2((scores - peak) * scale)
            total = jnp.sum(expo, axis=-1, keepdims=True)
            probs = (expo * (1.0 / total)).astype(jnp.bfloat16)
            mixed = jnp.dot(probs, all_ref[...], preferred_element_type=jnp.float32)
            for j in range(2):
                out = mixed[j * tokens : (j + 1) * tokens, :].T[HD:, :]
                out_ref[2 * (2 * step + i) + j] = out.astype(jnp.bfloat16)
        return carry

    lax.fori_loop(0, all_ref.shape[0] // (2 * block), attend, 0)


def early_projection(weight, pieces):
    rows = sum(piece.shape[0] for _, _, piece in pieces)
    return pl.pallas_call(
        project_body,
        out_shape=(
            pltpu.HBM((rows, 2 * HD), jnp.bfloat16),
            pltpu.HBM((HD, rows), jnp.bfloat16),
        ),
        in_specs=[VMEM] * (1 + len(pieces)),
        out_specs=(VMEM, VMEM),
        compiler_params=pltpu.CompilerParams(vmem_limit_bytes=8 << 20),
        cost_estimate=cost(6 * rows * HD * weight.shape[2]),
    )(weight, *(piece for _, _, piece in pieces))


def attended_heads(normed, w_qkv):
    cols = lax.axis_size("col")
    weight = w_qkv.transpose(0, 2, 1)
    tokens = normed.shape[0]
    pieces, (query_value, keys), mark = ring(normed, functools.partial(early_projection, weight))
    count = cols - 6
    early, late = pieces[:count], pieces[count:]
    body = functools.partial(
        attention_body,
        cols // 2,
        tokens,
        [(same, offset) for same, offset, _ in early],
        [(same, offset) for same, offset, _ in late],
    )
    heads = pl.pallas_call(
        body,
        out_shape=jax.ShapeDtypeStruct((cols, HD, tokens), jnp.bfloat16),
        in_specs=[pl.BlockSpec(memory_space=pltpu.SMEM), VMEM, HBM, HBM] + [VMEM] * len(late),
        out_specs=VMEM,
        scratch_shapes=[
            pltpu.VMEM((cols * tokens, 2 * HD), jnp.bfloat16),
            pltpu.VMEM((2 * HD, cols * tokens), jnp.bfloat16),
            pltpu.SemaphoreType.DMA((2, len(early))),
        ],
        compiler_params=pltpu.CompilerParams(vmem_limit_bytes=14 << 20),
        cost_estimate=cost(16 * HD * (cols * tokens) ** 2),
    )
    return heads(
        lax.axis_index("col").reshape(1),
        weight,
        pltpu.with_memory_space_constraint(query_value, pltpu.HBM),
        pltpu.with_memory_space_constraint(keys, pltpu.HBM),
        *(piece for _, _, piece in late)
    ), mark


def embed_body(
    half_ref, features_ref, gathered_ref, place_ref, own_ref, other_ref, left_ref, weight_ref, sems
):
    groups, per_group, channels, width = weight_ref.shape
    span = per_group * channels
    copies = [
        (
            pltpu.make_async_copy(
                features_ref.at[:, pl.ds(i * span, span)], left_ref.at[i], sems.at[0, i]
            ),
            pltpu.make_async_copy(
                gathered_ref.at[pl.ds(i * per_group, per_group), pl.ds(0, channels), :],
                weight_ref.at[i],
                sems.at[1, i],
            ),
        )
        for i in range(groups)
    ]
    for pair in copies:
        for copy in pair:
            copy.start()
    summed = jnp.zeros((features_ref.shape[0], width), jnp.float32)
    for i, pair in enumerate(copies):
        for copy in pair:
            copy.wait()
        summed = summed + jnp.dot(
            left_ref[i],
            weight_ref[i].reshape(span, width),
            preferred_element_type=jnp.float32,
        )
    columns, count, _ = place_ref.shape
    first_half = half_ref[0] == 0
    for column in range(columns):
        place = place_ref[column].astype(jnp.float32)
        first, second = (
            summed[(PAIR * column + image) * count :][:count] + place for image in range(PAIR)
        )
        part = slice(column * count, (column + 1) * count)
        own_ref[part, :] = jnp.where(first_half, first, second).astype(jnp.bfloat16)
        other_ref[part, :] = jnp.where(first_half, second, first).astype(jnp.bfloat16)


def embed(half, features, gathered, place):
    cols, _, width = gathered.shape
    groups = 4
    channels = features.shape[1] // cols
    out = jax.ShapeDtypeStruct((features.shape[0] // PAIR, width), jnp.bfloat16)
    return pl.pallas_call(
        embed_body,
        out_shape=(out, out),
        in_specs=[pl.BlockSpec(memory_space=pltpu.SMEM), HBM, HBM, VMEM],
        out_specs=(VMEM, VMEM),
        scratch_shapes=[
            pltpu.VMEM((groups, features.shape[0], features.shape[1] // groups), jnp.bfloat16),
            pltpu.VMEM((groups, cols // groups, channels, width), jnp.bfloat16),
            pltpu.SemaphoreType.DMA((2, groups)),
        ],
        compiler_params=pltpu.CompilerParams(vmem_limit_bytes=20 << 20),
        cost_estimate=cost(2 * features.size * width),
    )(half.reshape(1), features, gathered, place)


def out_body(member_ref, heads_ref, *refs):
    *weight_refs, tokens_ref, gain_ref, after_ref, normed_ref = refs
    cols, rows, half_width = weight_refs[0].shape
    rows = rows // PAIR
    sides = [0.0] * PAIR
    for step, weight_ref in enumerate(weight_refs):
        at = pl.multiple_of(jnp.bitwise_xor(member_ref[0], step) * rows, rows)
        heads = heads_ref[:, pl.ds(at, rows), :].reshape(cols * rows, -1)
        heads = heads.astype(jnp.float32).T.astype(jnp.bfloat16)
        for i in range(PAIR):
            weight = weight_ref[:, i * rows : (i + 1) * rows, :].reshape(cols * rows, half_width)
            sides[i] = sides[i] + jnp.dot(heads, weight, preferred_element_type=jnp.float32)
    after = tokens_ref[...].astype(jnp.float32) + jnp.concatenate(sides, axis=1)
    after_ref[...] = after
    normed_ref[...] = layer_norm(after, gain_ref[...]).astype(jnp.bfloat16)


def out_projection(member, heads, quarters, tokens_in, gain):
    width = tokens_in.shape[1]
    return pl.pallas_call(
        out_body,
        out_shape=(
            jax.ShapeDtypeStruct(tokens_in.shape, jnp.float32),
            jax.ShapeDtypeStruct(tokens_in.shape, jnp.bfloat16),
        ),
        in_specs=[pl.BlockSpec(memory_space=pltpu.SMEM)] + [VMEM] * (3 + len(quarters)),
        out_specs=(VMEM, VMEM),
        compiler_params=pltpu.CompilerParams(vmem_limit_bytes=10 << 20),
        cost_estimate=cost(2 * tokens_in.shape[0] * width * width),
    )(member.reshape(1), heads, *quarters, tokens_in, gain.reshape(1, width))


def mlp_body(first_ref, second_ref, gathered_ref, out_first_ref, out_second_ref, weight_ref, sems):
    groups, per_group, units, width = weight_ref.shape
    copies = [
        pltpu.make_async_copy(
            gathered_ref.at[pl.ds(i * per_group, per_group)], weight_ref.at[i], sems.at[i]
        )
        for i in range(groups)
    ]
    for copy in copies:
        copy.start()
    tokens = first_ref.shape[0]
    rows = jnp.concatenate([first_ref[...], second_ref[...]], axis=0)
    summed = jnp.zeros(rows.shape, jnp.float32)
    for i, copy in enumerate(copies):
        copy.wait()
        up = weight_ref[i, :, : units // 2, :].reshape(-1, width)
        down = weight_ref[i, :, units // 2 :, :].reshape(-1, width)
        hidden = jax.nn.gelu(matmul_nt(rows, up), approximate=True).astype(jnp.bfloat16)
        summed = summed + jnp.dot(hidden, down, preferred_element_type=jnp.float32)
    out_first_ref[...] = summed[:tokens].astype(out_first_ref.dtype)
    out_second_ref[...] = summed[tokens:].astype(out_second_ref.dtype)


def mlp_terms(first, second, gathered, first_type):
    cols, rows, width = gathered.shape
    groups = 4
    return pl.pallas_call(
        mlp_body,
        out_shape=(
            jax.ShapeDtypeStruct(first.shape, first_type),
            jax.ShapeDtypeStruct(first.shape, jnp.bfloat16),
        ),
        in_specs=[VMEM, VMEM, HBM],
        out_specs=(VMEM, VMEM),
        scratch_shapes=[
            pltpu.VMEM((groups, cols // groups, rows, width), jnp.bfloat16),
            pltpu.SemaphoreType.DMA((groups,)),
        ],
        compiler_params=pltpu.CompilerParams(vmem_limit_bytes=20 << 20),
        cost_estimate=cost(4 * first.shape[0] * width * cols * rows),
    )(first, second, gathered)


def on_device(
    images,
    stem_first,
    stem_conv,
    patch_weight,
    position,
    gain_attn,
    w_qkv,
    w_out,
    gain_mlp,
    w_up,
    w_down,
):
    member = lax.axis_index("row") % TEAM
    model_width = patch_weight.shape[1]
    hidden_here = w_down.shape[0] // TEAM
    half = lax.axis_index("row") % PAIR
    half_width = model_width // PAIR
    half_patch = lax.dynamic_slice_in_dim(patch_weight, half * half_width, half_width, 1)
    out_here = w_out.shape[0] // TEAM
    out_quarter = lax.dynamic_slice_in_dim(w_out, member * out_here, out_here, 0)
    first_shard = jnp.concatenate(
        [half_patch, out_quarter[:, :half_width], out_quarter[:, half_width:]], axis=0
    )
    first_weights = lax.all_gather(first_shard, "col", axis=0, tiled=False)
    strips, place = image_strips(images, position)
    packed = jnp.concatenate(
        [
            lax.dynamic_slice_in_dim(w_up.T, member * hidden_here, hidden_here, 0),
            lax.dynamic_slice_in_dim(w_down, member * hidden_here, hidden_here, 0),
        ],
        axis=0,
    )
    packed, strips = lax.optimization_barrier((packed, strips))
    cols_here = position.shape[0]
    features = stem_features(strips, images.shape[3], images.shape[4], stem_first, stem_conv)
    even = half == 0
    own, others = embed(
        half,
        pltpu.with_memory_space_constraint(features, pltpu.HBM),
        pltpu.with_memory_space_constraint(first_weights, pltpu.HBM),
        place,
    )
    others = lax.ppermute(others, "row", team_pairs(1))
    tokens_in = jnp.concatenate(
        [jnp.where(even, own, others), jnp.where(even, others, own)], axis=1
    )
    quarter = first_weights[:, half_patch.shape[0] :]
    quarter, tokens_in = lax.optimization_barrier((quarter, tokens_in))
    quarters = [quarter]
    for step in range(1, TEAM):
        quarters.append(lax.ppermute(quarter, "row", team_pairs(step)))
    normed = layer_norm(tokens_in.astype(jnp.float32), gain_attn).astype(jnp.bfloat16)
    heads, mark = attended_heads(normed, w_qkv)
    packed, mark = lax.optimization_barrier((packed, mark))
    gathered = lax.all_gather(packed, "col", axis=0, tiled=False)
    gathered = pltpu.with_memory_space_constraint(gathered, pltpu.HBM)
    heads_back = lax.all_to_all(heads, "col", 0, 0, tiled=True)
    after, normed_mlp = out_projection(
        member, heads_back, quarters, tokens_in, gain_mlp
    )
    near, far, farthest = (lax.ppermute(normed_mlp, "row", team_pairs(i)) for i in (1, 2, 3))
    own_term, near_term = mlp_terms(normed_mlp, near, gathered, jnp.float32)
    far, farthest, near_term = lax.optimization_barrier((far, farthest, near_term))
    near_back = lax.ppermute(near_term, "row", team_pairs(1))
    far_term, farthest_term = mlp_terms(far, farthest, gathered, jnp.bfloat16)
    encoded = after + own_term + near_back.astype(jnp.float32)
    for step, term in ((2, far_term), (3, farthest_term)):
        encoded = encoded + lax.ppermute(term, "row", team_pairs(step)).astype(jnp.float32)
    return encoded.astype(jnp.bfloat16).reshape(1, 1, cols_here, -1, model_width)


def solution(mesh):
    placed = (
        P("section", None, None, "row", "col"),
        P(),
        P(),
        P("col", None),
        P("col", "row", None),
        P(),
        P(None, None, "col"),
        P("col", None),
        P(),
        P(None, "col"),
        P("col", None),
    )
    return jax.shard_map(
        on_device,
        mesh=mesh,
        in_specs=placed,
        out_specs=P("section", "row", "col", None, None),
        check_vma=False,
    )
```

```python
import functools
import math

import jax
import jax.numpy as jnp
from jax import lax
from jax.experimental import pallas as pl
from jax.experimental.pallas import tpu as pltpu
from jax.sharding import PartitionSpec as P

HD = 64
TEAM = 4
PAIR = 2


def cost(flops):
    return pl.CostEstimate(flops=flops, bytes_accessed=flops // 256, transcendentals=0)


VMEM = pl.BlockSpec(memory_space=pltpu.VMEM)
HBM = pl.BlockSpec(memory_space=pltpu.HBM)


def layer_norm(vectors, gain_vec):
    row_mean = jnp.mean(vectors, axis=-1, keepdims=True)
    center = vectors - row_mean
    spread = jnp.mean(center * center, axis=-1, keepdims=True)
    return center * lax.rsqrt(spread + 1e-06) * gain_vec


def image_strips(images, position):
    sections = lax.axis_size("section")
    rows = lax.axis_size("row")
    pixels = images[0]
    img_count, colours, height, width = pixels.shape
    tile = height * width
    cols_here, rows_here, model_width = position.shape
    pixels = pixels.reshape(img_count // PAIR, 1, PAIR * colours, tile)
    pixels = jnp.broadcast_to(pixels, (img_count // PAIR, PAIR, PAIR * colours, tile))
    pixels = pixels.reshape(img_count, PAIR * colours, tile)
    place = position.reshape(cols_here * rows_here, model_width // tile, tile)
    place = place.transpose(1, 0, 2).reshape(-1, tile)
    place_rows = place.shape[0]
    slot_rows = PAIR * colours
    place = jnp.pad(place, ((0, slot_rows - place_rows), (0, 0)))
    here = lax.axis_index("section")
    slots = lax.broadcasted_iota(jnp.int32, (sections, 1, 1, 1), 0)
    outgoing = jnp.where(slots == here, place[None, None], pixels[None])
    outgoing = outgoing.reshape(sections * rows, slot_rows, tile)
    incoming = lax.all_to_all(outgoing, ("section", "row"), 0, 0, tiled=True)
    other = (here + 1) % sections
    strips = lax.dynamic_slice_in_dim(incoming, other * rows, rows, 0)
    strips = strips.reshape(rows, PAIR, colours, tile).transpose(1, 0, 2, 3)
    place = lax.dynamic_slice_in_dim(incoming, here * rows, rows, 0)
    half_rows = place_rows // PAIR
    member = lax.axis_index("row") % PAIR
    place = lax.dynamic_slice_in_dim(place, member * half_rows, half_rows, 1)
    place = place.reshape(rows, -1, cols_here, rows_here, tile).transpose(2, 0, 3, 1, 4)
    return strips, place.reshape(cols_here, rows * rows_here, -1)


def moved(value, step):
    count = lax.axis_size("col")
    return lax.ppermute(value, "col", [(i, (i + step) % count) for i in range(count)])


def core_swapped(value):
    return lax.ppermute(value, "col", [(i, i ^ 1) for i in range(lax.axis_size("col"))])


def ring(shard, early_work):
    chips = lax.axis_size("col") // 2
    steps = chips // 2
    pieces = [(True, 0, shard), (False, 0, core_swapped(shard))]
    below, above = shard, shard
    for step in range(1, steps):
        if step > 2:
            below, above, first, second = lax.optimization_barrier(
                (below, above, pieces[-6][2], pieces[-5][2])
            )
            pieces[-6] = (*pieces[-6][:2], first)
            pieces[-5] = (*pieces[-5][:2], second)
        below, above = moved(below, 2), moved(above, -2)
        pieces += [
            (False, chips - step, core_swapped(below)),
            (False, step, core_swapped(above)),
            (True, chips - step, below),
            (True, step, above),
        ]
    done = early_work(pieces[:-4])
    below, above, done = lax.optimization_barrier((below, above, done))
    pieces[-1] = (True, steps - 1, above)
    count = lax.axis_size("col")
    last = lax.ppermute(
        jnp.where(lax.axis_index("col") % 2 == 0, below, above),
        "col",
        [(i, (i + (2 if i % 2 == 0 else -2)) % count) for i in range(count)],
    )
    pieces += [(True, steps, last), (False, steps, core_swapped(last))]
    return pieces, done, above


def stem_body(parts, *refs):
    first_refs = refs[:parts]
    low_ref, high_ref, first_weight_ref, conv_ref, out_ref = refs[parts : parts + 5]
    planes_ref, weight_ref, done_ref, low_refs, high_refs, sems = refs[parts + 5 :]
    images, pixels, lanes = first_refs[0].shape
    fetch = pltpu.make_async_copy(conv_ref, weight_ref, sems.at[16])
    fetch.start()
    low_refs = [low_refs.at[i] for i in range(parts)]
    high_refs = [high_refs.at[i] for i in range(parts)]
    for side_ref, side_refs in ((low_ref, low_refs), (high_ref, high_refs)):
        side = jnp.dot(
            side_ref[...].astype(jnp.float32).T.astype(jnp.bfloat16),
            first_weight_ref[...],
            preferred_element_type=jnp.float32,
        )
        side = jnp.maximum(side, 0.0).astype(jnp.bfloat16).astype(jnp.float32)
        for i, ref in enumerate(side_refs):
            ref[...] = side[:, i * lanes : (i + 1) * lanes].reshape(images, -1, lanes)
    width = 16
    count = pixels // (4 * width)
    row = lax.broadcasted_iota(jnp.int32, (count, parts * lanes), 0)
    group = images * count

    def put(a, b, slot, image, values):
        at = pl.multiple_of(slot * group + image * count, count)
        planes_ref[a + 1, b, pl.ds(at, count), :] = values.astype(jnp.bfloat16)
        if a == 3:
            moved_down = jnp.where(row == 0, 0.0, pltpu.roll(values, 1, 0))
            planes_ref[0, b, pl.ds(at, count), :] = moved_down.astype(jnp.bfloat16)
        if a == 0:
            moved_up = jnp.where(row == count - 1, 0.0, pltpu.roll(values, count - 1, 0))
            planes_ref[5, b, pl.ds(at, count), :] = moved_up.astype(jnp.bfloat16)

    def strided(part_refs, image, start, stride):
        return jnp.concatenate(
            [ref[image, pl.ds(start, count, stride=stride), :] for ref in part_refs], axis=1
        )

    def build(column, carry):
        j, b = column // 4, column % 4
        for image in range(images):
            for a in range(4):
                put(a, b, j + 1, image, strided(first_refs, image, width * a + column, 4 * width))
        return carry

    lax.fori_loop(0, width, build, 0)
    for image in range(images):
        for a in range(4):
            put(a, 3, 0, image, strided(low_refs, image, a, 4))
            put(a, 0, width // 4 + 1, image, strided(high_refs, image, a, 4))

    rows = width // 4 * group
    channels = out_ref.shape[1] // 16

    def sent(phase):
        at = pl.multiple_of(phase * channels, channels)
        return pltpu.make_async_copy(
            done_ref.at[phase], out_ref.at[:, pl.ds(at, channels)], sems.at[phase]
        )

    fetch.wait()

    def convolve(phase, carry):
        a, b = phase // 4, phase % 4
        summed = planes_ref[a + 1, b, group : group + rows, :].astype(jnp.float32)
        for tap_a in range(3):
            for tap_b in range(3):
                column = b + tap_b + 3
                at = pl.multiple_of((column // 4) * group, group)
                window = planes_ref[a + tap_a, column % 4, pl.ds(at, rows), :]
                summed = summed + jnp.dot(
                    window, weight_ref[tap_a, tap_b], preferred_element_type=jnp.float32
                )
        done_ref[phase] = jnp.maximum(summed, 0.0).astype(jnp.bfloat16)
        sent(phase).start()
        return carry

    lax.fori_loop(0, 16, convolve, 0)
    for phase in range(16):
        sent(phase).wait()


def stem_features(strips, height, width, stem_first, stem_conv):
    images, parts, colours, _ = strips.shape
    total = parts * height
    channels = stem_first.shape[1]
    by_column = strips.reshape(images, parts, colours, height, width)

    def column(at):
        return by_column[:, :, :, :, at].transpose(2, 0, 1, 3).reshape(colours, images * total)

    count = lax.axis_size("col")
    forward = [(i, i + 1) for i in range(count - 1)]
    backward = [(target, source) for source, target in forward]
    low = lax.ppermute(column(width - 1), "col", forward)
    high = lax.ppermute(column(0), "col", backward)

    lanes = 128
    starts = range(0, channels, lanes)

    def first_of(values, spec, start):
        result = jnp.einsum(
            spec, values, stem_first[:, start : start + lanes], preferred_element_type=jnp.float32
        )
        result = lax.reduce_precision(jnp.maximum(result, 0.0), 8, 7)
        return result.reshape(images, -1, lanes)

    firsts = [first_of(strips, "mrkp,kc->mrpc", start) for start in starts]
    tokens = images * total * width // 16
    return pl.pallas_call(
        functools.partial(stem_body, len(starts)),
        out_shape=pltpu.HBM((tokens, 16 * channels), jnp.bfloat16),
        in_specs=[VMEM] * (len(starts) + 3) + [HBM],
        out_specs=HBM,
        scratch_shapes=[
            pltpu.VMEM((6, 4, (width // 4 + 2) * images * total // 4, channels), jnp.bfloat16),
            pltpu.VMEM(stem_conv.shape, jnp.bfloat16),
            pltpu.VMEM((16, tokens, channels), jnp.bfloat16),
            pltpu.VMEM((len(starts), images, total, lanes), jnp.float32),
            pltpu.VMEM((len(starts), images, total, lanes), jnp.float32),
            pltpu.SemaphoreType.DMA((17,)),
        ],
        compiler_params=pltpu.CompilerParams(vmem_limit_bytes=20 << 20),
        cost_estimate=cost(18 * images * total * width * channels**2),
    )(
        *firsts,
        low,
        high,
        stem_first,
        pltpu.with_memory_space_constraint(stem_conv, pltpu.HBM),
    )


def team_pairs(step):
    return [(i, i ^ step) for i in range(lax.axis_size("row"))]


def matmul_nt(left, right):
    return lax.dot_general(
        left, right, (((1,), (1,)), ((), ())), preferred_element_type=jnp.float32
    )


def project(rows, weight_ref):
    pair = jnp.concatenate([weight_ref[0], weight_ref[2]], axis=0)
    query_value = matmul_nt(rows, pair).astype(jnp.bfloat16)
    keys = matmul_nt(weight_ref[1], rows).astype(jnp.bfloat16)
    return query_value, keys


def project_body(weight_ref, *refs):
    *piece_refs, query_value_ref, key_ref = refs
    start = 0
    for piece_ref in piece_refs:
        count = piece_ref.shape[0]
        query_value, keys = project(piece_ref[...], weight_ref)
        query_value_ref[start : start + count] = query_value
        key_ref[:, start : start + count] = keys
        start += count


def attention_body(chips, tokens, early, late, place_ref, weight_ref, qv_ref, early_key_ref, *refs):
    *piece_refs, out_ref, all_ref, key_ref, done_ref, sems, out_sems = refs
    place = place_ref[0]
    chip, core = place // 2, place % 2
    key_ref[HD:, :] = jnp.zeros((HD, key_ref.shape[1]), key_ref.dtype)

    def places(same, offset):
        at = 2 * lax.rem(chip + offset, chips) + (core if same else 1 - core)
        at = pl.ds(pl.multiple_of(at * tokens, tokens), tokens)
        return all_ref.at[at, :], key_ref.at[pl.ds(0, HD), at]

    copies = []
    for i, (same, offset) in enumerate(early):
        part = pl.ds(i * tokens, tokens)
        query_value, keys = places(same, offset)
        copies += [
            pltpu.make_async_copy(qv_ref.at[part, :], query_value, sems.at[0, i]),
            pltpu.make_async_copy(early_key_ref.at[:, part], keys, sems.at[1, i]),
        ]
    for copy in copies:
        copy.start()
    for (same, offset), piece_ref in zip(late, piece_refs, strict=True):
        for ref, values in zip(
            places(same, offset), project(piece_ref[...], weight_ref), strict=True
        ):
            ref[...] = values
    for copy in copies:
        copy.wait()

    block = 2 * tokens
    scale = HD ** (-0.5) * math.log2(math.e)

    def sent(target):
        return pltpu.make_async_copy(done_ref.at[target], out_ref.at[target], out_sems.at[target])

    def attend(step, carry):
        for i in range(2):
            at = pl.multiple_of((2 * step + i) * block, block)
            scores = jnp.dot(
                all_ref[pl.ds(at, block), :], key_ref[...], preferred_element_type=jnp.float32
            )
            peak = jnp.max(scores, axis=-1, keepdims=True)
            expo = jnp.exp2((scores - peak) * scale)
            total = jnp.sum(expo, axis=-1, keepdims=True)
            probs = (expo * (1.0 / total)).astype(jnp.bfloat16)
            mixed = jnp.dot(probs, all_ref[...], preferred_element_type=jnp.float32)
            for j in range(2):
                out = mixed[j * tokens : (j + 1) * tokens, :].T[HD:, :]
                target = 2 * (2 * step + i) + j
                done_ref[target] = out.astype(jnp.bfloat16)
                sent(target).start()
        return carry

    lax.fori_loop(0, all_ref.shape[0] // (2 * block), attend, 0)
    for target in range(out_ref.shape[0]):
        sent(target).wait()


def early_projection(weight, pieces):
    rows = sum(piece.shape[0] for _, _, piece in pieces)
    return pl.pallas_call(
        project_body,
        out_shape=(
            pltpu.HBM((rows, 2 * HD), jnp.bfloat16),
            pltpu.HBM((HD, rows), jnp.bfloat16),
        ),
        in_specs=[VMEM] * (1 + len(pieces)),
        out_specs=(VMEM, VMEM),
        compiler_params=pltpu.CompilerParams(vmem_limit_bytes=8 << 20),
        cost_estimate=cost(6 * rows * HD * weight.shape[2]),
    )(weight, *(piece for _, _, piece in pieces))


def attended_heads(normed, w_qkv):
    cols = lax.axis_size("col")
    weight = w_qkv.transpose(0, 2, 1)
    tokens = normed.shape[0]
    pieces, (query_value, keys), mark = ring(normed, functools.partial(early_projection, weight))
    count = cols - 6
    early, late = pieces[:count], pieces[count:]
    body = functools.partial(
        attention_body,
        cols // 2,
        tokens,
        [(same, offset) for same, offset, _ in early],
        [(same, offset) for same, offset, _ in late],
    )
    heads = pl.pallas_call(
        body,
        out_shape=pltpu.HBM((cols, HD, tokens), jnp.bfloat16),
        in_specs=[pl.BlockSpec(memory_space=pltpu.SMEM), VMEM, HBM, HBM] + [VMEM] * len(late),
        out_specs=HBM,
        scratch_shapes=[
            pltpu.VMEM((cols * tokens, 2 * HD), jnp.bfloat16),
            pltpu.VMEM((2 * HD, cols * tokens), jnp.bfloat16),
            pltpu.VMEM((cols, HD, tokens), jnp.bfloat16),
            pltpu.SemaphoreType.DMA((2, len(early))),
            pltpu.SemaphoreType.DMA((cols,)),
        ],
        compiler_params=pltpu.CompilerParams(vmem_limit_bytes=14 << 20),
        cost_estimate=cost(16 * HD * (cols * tokens) ** 2),
    )
    return heads(
        lax.axis_index("col").reshape(1),
        weight,
        pltpu.with_memory_space_constraint(query_value, pltpu.HBM),
        pltpu.with_memory_space_constraint(keys, pltpu.HBM),
        *(piece for _, _, piece in late)
    ), mark


def embed_body(
    half_ref, features_ref, gathered_ref, place_ref, own_ref, other_ref, left_ref, weight_ref, sems
):
    groups, per_group, channels, width = weight_ref.shape
    span = per_group * channels
    copies = [
        (
            pltpu.make_async_copy(
                features_ref.at[:, pl.ds(i * span, span)], left_ref.at[i], sems.at[0, i]
            ),
            pltpu.make_async_copy(
                gathered_ref.at[pl.ds(i * per_group, per_group), pl.ds(0, channels), :],
                weight_ref.at[i],
                sems.at[1, i],
            ),
        )
        for i in range(groups)
    ]
    for pair in copies:
        for copy in pair:
            copy.start()
    summed = jnp.zeros((features_ref.shape[0], width), jnp.float32)
    for i, pair in enumerate(copies):
        for copy in pair:
            copy.wait()
        summed = summed + jnp.dot(
            left_ref[i],
            weight_ref[i].reshape(span, width),
            preferred_element_type=jnp.float32,
        )
    columns, count, _ = place_ref.shape
    first_half = half_ref[0] == 0
    for column in range(columns):
        place = place_ref[column].astype(jnp.float32)
        first, second = (
            summed[(PAIR * column + image) * count :][:count] + place for image in range(PAIR)
        )
        part = slice(column * count, (column + 1) * count)
        own_ref[part, :] = jnp.where(first_half, first, second).astype(jnp.bfloat16)
        other_ref[part, :] = jnp.where(first_half, second, first).astype(jnp.bfloat16)


def embed(half, features, gathered, place):
    cols, _, width = gathered.shape
    groups = 4
    channels = features.shape[1] // cols
    out = jax.ShapeDtypeStruct((features.shape[0] // PAIR, width), jnp.bfloat16)
    return pl.pallas_call(
        embed_body,
        out_shape=(out, out),
        in_specs=[pl.BlockSpec(memory_space=pltpu.SMEM), HBM, HBM, VMEM],
        out_specs=(VMEM, VMEM),
        scratch_shapes=[
            pltpu.VMEM((groups, features.shape[0], features.shape[1] // groups), jnp.bfloat16),
            pltpu.VMEM((groups, cols // groups, channels, width), jnp.bfloat16),
            pltpu.SemaphoreType.DMA((2, groups)),
        ],
        compiler_params=pltpu.CompilerParams(vmem_limit_bytes=20 << 20),
        cost_estimate=cost(2 * features.size * width),
    )(half.reshape(1), features, gathered, place)


def out_body(member_ref, heads_ref, *refs):
    *weight_refs, tokens_ref, gain_ref, after_ref, normed_ref = refs
    cols, rows, half_width = weight_refs[0].shape
    rows = rows // PAIR
    sides = [0.0] * PAIR
    for step, weight_ref in enumerate(weight_refs):
        at = pl.multiple_of(jnp.bitwise_xor(member_ref[0], step) * rows, rows)
        heads = heads_ref[:, pl.ds(at, rows), :].reshape(cols * rows, -1)
        heads = heads.astype(jnp.float32).T.astype(jnp.bfloat16)
        for i in range(PAIR):
            weight = weight_ref[:, i * rows : (i + 1) * rows, :].reshape(cols * rows, half_width)
            sides[i] = sides[i] + jnp.dot(heads, weight, preferred_element_type=jnp.float32)
    after = tokens_ref[...].astype(jnp.float32) + jnp.concatenate(sides, axis=1)
    after_ref[...] = after
    normed_ref[...] = layer_norm(after, gain_ref[...]).astype(jnp.bfloat16)


def out_projection(member, heads, quarters, tokens_in, gain):
    width = tokens_in.shape[1]
    return pl.pallas_call(
        out_body,
        out_shape=(
            pltpu.HBM(tokens_in.shape, jnp.float32),
            jax.ShapeDtypeStruct(tokens_in.shape, jnp.bfloat16),
        ),
        in_specs=[pl.BlockSpec(memory_space=pltpu.SMEM)] + [VMEM] * (3 + len(quarters)),
        out_specs=(VMEM, VMEM),
        compiler_params=pltpu.CompilerParams(vmem_limit_bytes=10 << 20),
        cost_estimate=cost(2 * tokens_in.shape[0] * width * width),
    )(member.reshape(1), heads, *quarters, tokens_in, gain.reshape(1, width))


def mlp_body(first_ref, second_ref, gathered_ref, out_first_ref, out_second_ref, weight_ref, sems):
    groups, per_group, units, width = weight_ref.shape
    copies = [
        pltpu.make_async_copy(
            gathered_ref.at[pl.ds(i * per_group, per_group)], weight_ref.at[i], sems.at[i]
        )
        for i in range(groups)
    ]
    for copy in copies:
        copy.start()
    tokens = first_ref.shape[0]
    rows = jnp.concatenate([first_ref[...], second_ref[...]], axis=0)
    summed = jnp.zeros(rows.shape, jnp.float32)
    for i, copy in enumerate(copies):
        copy.wait()
        up = weight_ref[i, :, : units // 2, :].reshape(-1, width)
        down = weight_ref[i, :, units // 2 :, :].reshape(-1, width)
        hidden = jax.nn.gelu(matmul_nt(rows, up), approximate=True).astype(jnp.bfloat16)
        summed = summed + jnp.dot(hidden, down, preferred_element_type=jnp.float32)
    out_first_ref[...] = summed[:tokens].astype(out_first_ref.dtype)
    out_second_ref[...] = summed[tokens:].astype(out_second_ref.dtype)


def mlp_terms(first, second, gathered, first_type):
    cols, rows, width = gathered.shape
    groups = 4
    return pl.pallas_call(
        mlp_body,
        out_shape=(
            jax.ShapeDtypeStruct(first.shape, first_type),
            jax.ShapeDtypeStruct(first.shape, jnp.bfloat16),
        ),
        in_specs=[VMEM, VMEM, HBM],
        out_specs=(VMEM, VMEM),
        scratch_shapes=[
            pltpu.VMEM((groups, cols // groups, rows, width), jnp.bfloat16),
            pltpu.SemaphoreType.DMA((groups,)),
        ],
        compiler_params=pltpu.CompilerParams(vmem_limit_bytes=20 << 20),
        cost_estimate=cost(4 * first.shape[0] * width * cols * rows),
    )(first, second, gathered)


def on_device(
    images,
    stem_first,
    stem_conv,
    patch_weight,
    position,
    gain_attn,
    w_qkv,
    w_out,
    gain_mlp,
    w_up,
    w_down,
):
    member = lax.axis_index("row") % TEAM
    model_width = patch_weight.shape[1]
    hidden_here = w_down.shape[0] // TEAM
    half = lax.axis_index("row") % PAIR
    half_width = model_width // PAIR
    half_patch = lax.dynamic_slice_in_dim(patch_weight, half * half_width, half_width, 1)
    out_here = w_out.shape[0] // TEAM
    out_quarter = lax.dynamic_slice_in_dim(w_out, member * out_here, out_here, 0)
    first_shard = jnp.concatenate(
        [half_patch, out_quarter[:, :half_width], out_quarter[:, half_width:]], axis=0
    )
    first_weights = lax.all_gather(first_shard, "col", axis=0, tiled=False)
    strips, place = image_strips(images, position)
    packed = jnp.concatenate(
        [
            lax.dynamic_slice_in_dim(w_up.T, member * hidden_here, hidden_here, 0),
            lax.dynamic_slice_in_dim(w_down, member * hidden_here, hidden_here, 0),
        ],
        axis=0,
    )
    packed, strips = lax.optimization_barrier((packed, strips))
    cols_here = position.shape[0]
    features = stem_features(strips, images.shape[3], images.shape[4], stem_first, stem_conv)
    even = half == 0
    own, others = embed(
        half,
        pltpu.with_memory_space_constraint(features, pltpu.HBM),
        pltpu.with_memory_space_constraint(first_weights, pltpu.HBM),
        place,
    )
    others = lax.ppermute(others, "row", team_pairs(1))
    tokens_in = jnp.concatenate(
        [jnp.where(even, own, others), jnp.where(even, others, own)], axis=1
    )
    quarter = first_weights[:, half_patch.shape[0] :]
    quarter, tokens_in = lax.optimization_barrier((quarter, tokens_in))
    quarters = [quarter]
    for step in range(1, TEAM):
        quarters.append(lax.ppermute(quarter, "row", team_pairs(step)))
    normed = layer_norm(tokens_in.astype(jnp.float32), gain_attn).astype(jnp.bfloat16)
    heads, mark = attended_heads(normed, w_qkv)
    packed, mark = lax.optimization_barrier((packed, mark))
    gathered = lax.all_gather(packed, "col", axis=0, tiled=False)
    gathered = pltpu.with_memory_space_constraint(gathered, pltpu.HBM)
    heads_back = lax.all_to_all(heads, "col", 0, 0, tiled=True)
    after, normed_mlp = out_projection(
        member, heads_back, quarters, tokens_in, gain_mlp
    )
    near, far, farthest = (lax.ppermute(normed_mlp, "row", team_pairs(i)) for i in (1, 2, 3))
    own_term, near_term = mlp_terms(normed_mlp, near, gathered, jnp.float32)
    far, farthest, near_term = lax.optimization_barrier((far, farthest, near_term))
    near_back = lax.ppermute(near_term, "row", team_pairs(1))
    far_term, farthest_term = mlp_terms(far, farthest, gathered, jnp.bfloat16)
    encoded = after + own_term + near_back.astype(jnp.float32)
    for step, term in ((2, far_term), (3, farthest_term)):
        encoded = encoded + lax.ppermute(term, "row", team_pairs(step)).astype(jnp.float32)
    return encoded.astype(jnp.bfloat16).reshape(1, 1, cols_here, -1, model_width)


def solution(mesh):
    placed = (
        P("section", None, None, "row", "col"),
        P(),
        P(),
        P("col", None),
        P("col", "row", None),
        P(),
        P(None, None, "col"),
        P("col", None),
        P(),
        P(None, "col"),
        P("col", None),
    )
    return jax.shard_map(
        on_device,
        mesh=mesh,
        in_specs=placed,
        out_specs=P("section", "row", "col", None, None),
        check_vma=False,
    )
```
